32 devices in a mesh: gx: 4 (over y, core), gy: 8 (over z, x).
Axes of the slice: x: 2, y: 2, z: 4, core: 2. Of those that a mesh axis runs over, the one named last changes fastest.
Arguments:
- disp: float32 [3, 32, 128, 128], P(None, 'gx', 'gy'), may hold values from -3 to 3
- vel: float32 [3, 32, 128, 128], P(None, 'gx', 'gy'), may hold values from -30 to 30
- load: float32 [3, 32, 128, 128], P(None, 'gx', 'gy'), may hold values from -96 to 96
- flags: int32 [32, 128, 128], P('gx', 'gy'), may hold values 0 or 1
- mask_bits: int32 [4, 32, 128, 128], P(None, 'gx', 'gy'), may hold values from 0 to 2147483647, as said below
Outputs:
- disp_out: float32 [3, 32, 128, 128], P(None, 'gx', 'gy')
- vel_out: float32 [3, 32, 128, 128], P(None, 'gx', 'gy')
The draws below stay inside these ranges and needn't reach their ends.
Inputs may be any that keep to these rules, and one draw needn't show every extreme that they name: `mask_bits`: bit b (0 to 30) of word w marks the cell's bond to neighbour number 31 w + b as broken; bit 31, and bits of numbers 122 and above, are zero.
All inputs are finite; a program needn't handle non-finite values. No bound on the sum of `flags` on one device may be relied on, other than what follows from the above.
Results may differ from the reference program's by a relative error of at most 0.0001.
Values sent between devices are 32-bit elements; how exact they have to be, the bound alone decides.
A program may use at most 128 MiB of HBM per device.

```python
import math
import jax
import jax.numpy as jnp
from jax import lax

NZ = 128
ITERS = 8
NX = 32
NY = 128


def neighbour_table_drawn():
    table = []
    for across in range(-3, 4):
        for along in range(-3, 4):
            for upward in range(-3, 4):
                length = across * across + along * along + upward * upward
                if 0 < length <= 9:
                    table.append((across, along, upward))
    return table


def draw_vel(key, part):
    places_x = jnp.arange(NX, dtype=jnp.float32) / max(NX - 1, 1)
    places_y = jnp.arange(NY, dtype=jnp.float32) / max(NY - 1, 1)
    amplitude = 0.3 * (1.0 + 2.0 * places_x)[:, None, None] * (1.0 + 2.0 * places_y)[None, :, None]
    first = jax.random.fold_in(key, 11)
    base = jnp.clip(jax.random.normal(first, (3, NX, NY, NZ), jnp.float32), -4.0, 4.0)
    return (amplitude[None] * base).astype(jnp.float32)


def draw_mask_bits(key, part):
    table = neighbour_table_drawn()
    places_x = jnp.arange(NX, dtype=jnp.int32)[:, None, None]
    places_y = jnp.arange(NY, dtype=jnp.int32)[None, :, None]
    middle = NX // 2
    words = []
    for word in range(4):
        packed = jnp.zeros((NX, NY, NZ), jnp.int32)
        for bit in range(31):
            number = 31 * word + bit
            if number < 122:
                across = table[number][0]
                coin = jax.random.randint(jax.random.fold_in(key, 100 + number), (NX, NY, NZ), 0, 16)
                crosses = (places_x < middle) & (places_x + across >= middle) | (places_x >= middle) & (places_x + across < middle)
                crack = crosses & (places_y < NY // 2)
                broken = (coin == 0) | crack
                packed = packed | broken.astype(jnp.int32) << bit
        words.append(packed)
    return jnp.stack(words)


def set_ends(array, rng, low, high):
    index_at = [jax.random.randint(jax.random.fold_in(rng, axis), (), 0, length) for axis, length in enumerate(array.shape)]
    widest = array.shape.index(max(array.shape))
    next_to = index_at[:widest] + [(index_at[widest] + 1) % array.shape[widest]] + index_at[widest + 1:]
    return array.at[tuple(index_at)].set(low).at[tuple(next_to)].set(high)


def level_of(rng, dims, split, low, high):
    factor_of = 1.0
    for dim, shards_of in split:
        steps = jax.random.uniform(jax.random.fold_in(jax.random.fold_in(rng, 6), dim), (shards_of,), jnp.float32, low / len(split), high / len(split))
        factor_of = factor_of * jnp.repeat(jnp.exp(steps), dims[dim] // shards_of).reshape((-1,) + (1,) * (len(dims) - 1 - dim))
    return factor_of


def scatter_about(own_key, dims, spread, bound, split=(), kind=jnp.bfloat16):
    factor_of = level_of(own_key, dims, split, -0.22, 0.18) if split else 1.0
    entries = jax.random.normal(own_key, dims, jnp.float32) * spread * factor_of
    return jnp.minimum(jnp.maximum(entries, -bound), bound).astype(kind)


def setup_inputs(seed: int = 0) -> dict:
    key_of = jax.random.split(jax.random.key(seed), 6)
    return {
        "disp": scatter_about(key_of[0], (3, NX, NY, NZ), 0.5, 3.0, ((1, 4), (2, 8)), jnp.float32),
        "vel": draw_vel(jax.random.fold_in(key_of[5], 71), 0),
        "load": scatter_about(key_of[2], (3, NX, NY, NZ), 16.0, 96.0, ((1, 4), (2, 8)), jnp.float32),
        "flags": set_ends((jax.random.randint(key_of[3], (NX, NY, NZ), 0, 3) < 1).astype(jnp.int32), jax.random.fold_in(key_of[3], 1), 0, 1),
        "mask_bits": draw_mask_bits(jax.random.fold_in(key_of[5], 71), 0),
    }


fictive_mass = 64.0
epsilon = 1e-06

def neighbour_table():
    table = []
    for across in range(-3, 4):
        for along in range(-3, 4):
            for upward in range(-3, 4):
                length = across * across + along * along + upward * upward
                if 0 < length <= 9:
                    table.append((across, along, upward))
    return table

def bond_forces(field_pad, words, words_pad, exist_pad):
    rows = words.shape[1]
    cols = words.shape[2]
    depth = words.shape[3]
    centre = field_pad[:, 3:3 + rows, 3:3 + cols, 3:3 + depth]
    totals = [jnp.zeros((rows, cols, depth), jnp.float32) for index in range(3)]
    for number, offset in enumerate(neighbour_table()):
        across, along, upward = offset
        word, bit = divmod(number, 31)
        mirror_word, mirror_bit = divmod(121 - number, 31)
        window = (slice(3 + across, 3 + across + rows), slice(3 + along, 3 + along + cols), slice(3 + upward, 3 + upward + depth))
        other = field_pad[(slice(None),) + window]
        own_flag = words[word] >> bit & 1
        far_flag = words_pad[mirror_word][window] >> mirror_bit & 1
        intact = (own_flag | far_flag == 0) & (exist_pad[window] > 0)
        length = float(across * across + along * along + upward * upward)
        weight = 1.0 / (length * math.sqrt(length))
        stretch = float(across) * (other[0] - centre[0]) + float(along) * (other[1] - centre[1]) + float(upward) * (other[2] - centre[2])
        scaled = jnp.where(intact, stretch * weight, jnp.float32(0.0))
        totals[0] = totals[0] + float(across) * scaled
        totals[1] = totals[1] + float(along) * scaled
        totals[2] = totals[2] + float(upward) * scaled
    return jnp.stack(totals)

def reference(disp, vel, load, flags, mask_bits):
    words_pad = jnp.pad(mask_bits, ((0, 0), (3, 3), (3, 3), (3, 3)))
    exist_pad = jnp.pad(jnp.ones(mask_bits.shape[1:], jnp.int32), 3)
    applied = flags.astype(jnp.float32)[None] * load
    count = 3.0 * NX * NY * NZ

    def internal(field):
        field_pad = jnp.pad(field, ((0, 0), (3, 3), (3, 3), (3, 3)))
        return bond_forces(field_pad, mask_bits, words_pad, exist_pad)
    previous = lax.fori_loop(0, 1, lambda index, carry: internal(disp - vel), jnp.zeros_like(disp))

    def relax(index, state):
        field, speed, before = state
        current = internal(field)
        total = current + applied
        kinetic = jnp.sum(speed * speed)
        rayleigh = jnp.sum(speed * (before - current))
        damping = 2.0 * jnp.sqrt(rayleigh / count / (fictive_mass * (kinetic / count + epsilon)))
        alpha = (2.0 - damping) / (2.0 + damping)
        beta = 2.0 / (fictive_mass * (2.0 + damping))
        speed = alpha * speed + beta * total
        return (field + speed, speed, current)
    field, speed, before = lax.fori_loop(0, ITERS, relax, (disp, vel, previous))
    return (field, speed)
```

```python
import functools
import math

import jax
import jax.numpy as jnp
from jax import lax
from jax.experimental import pallas as pl
from jax.experimental.pallas import tpu as pltpu
from jax.sharding import PartitionSpec as P

ITERS = 8
MESH = pl.DeviceIdType.MESH

fictive_mass = 64.0
epsilon = 1e-06

EDGE = 8
SLOTS = 4


def neighbour_table():
    table = []
    for across in range(-3, 4):
        for along in range(-3, 4):
            for upward in range(-3, 4):
                length = across * across + along * along + upward * upward
                if 0 < length <= 9:
                    table.append((across, along, upward))
    return table


TABLE = neighbour_table()
NUMBER = {offset: number for number, offset in enumerate(TABLE)}

PLANES = [(1, 0), (1, 1), (2, 0)]
LONG = [(1, 2), (2, 1), (3, 0)]


def reach(along, upward):
    return [a for a in range(-3, 4) if (a, along, upward) in NUMBER]


def crossing(layer, r):
    far = layer + r
    return [(p, c) for c in range(-2, 3) for p in range(-2, 3) if far * far + p * p + c * c <= 9]


FACE = {}
for plane in PLANES:
    for offset in crossing(*plane):
        FACE[plane + offset] = len(FACE)
for plane in LONG:
    FACE[plane + (0, 0)] = len(FACE)


def bond(offset):
    number = NUMBER[offset]
    word, bit = divmod(number, 31)
    mirror_word, mirror_bit = divmod(121 - number, 31)
    length = float(sum(part * part for part in offset))
    return word, 1 << bit, mirror_word, 1 << mirror_bit, 1.0 / (length * math.sqrt(length))


def rolled(cells, upward):
    depth = cells.shape[-1]
    if upward == 0:
        return cells
    return pltpu.roll(cells, (-upward) % depth, cells.ndim - 1)


def add(total, term):
    return term if total is None else total + term


def scaled(scale, value):
    return value if scale == 1 else float(scale) * value


def kernel(
    nx, ny,
    disp_in, vel_in, load_in, flags_in, mask_in,
    field, speed,
    load, flags, mask,
    weights, diagonal, pad, mask_pad, shifted, mask_shifted, mixed, plain, force, total, change,
    wx, wy, xg, xw, yg, yw, xr, yr, mxr, myr, mx3, my3,
    xpack, ypack, xslot, yslot, mxpack, mypack, my3pack, mxslot, myslot, my3slot,
    acc, ab, sums_out, sums_in,
    local_sem, send_sem, recv_sem, msend_sem, mrecv_sem, sum_send_sem, sum_recv_sem, ready,
):
    depth = flags.shape[-1]
    cells = flags.shape[0]
    rows = pad.shape[1] - 6
    cols = cells // rows
    count = 3.0 * rows * nx * cols * ny * depth
    devices = nx * ny
    my_x = lax.axis_index("gx")
    my_y = lax.axis_index("gy")
    f32, i32 = jnp.float32, jnp.int32

    fetches = [
        pltpu.make_async_copy(src, dst, local_sem.at[index])
        for index, (src, dst) in enumerate((
            (mask_in, mask), (disp_in, field), (vel_in, speed), (load_in, load), (flags_in, flags),
        ))
    ]
    for fetch in fetches:
        fetch.start()

    sides = []
    for step_x, step_y in ((-1, 0), (1, 0), (0, -1), (0, 1), (-1, -1), (-1, 1), (1, -1), (1, 1)):
        there = None
        for step, mine, size in ((step_x, my_x, nx), (step_y, my_y, ny)):
            if step:
                near = mine > 0 if step < 0 else mine < size - 1
                there = near if there is None else there & near
        sides.append((step_x, step_y, there))

    barrier = pltpu.get_barrier_semaphore()
    peers = nx + ny - 2
    for step_x, step_y, there in sides[4:]:
        @pl.when(there)
        def _():
            pl.semaphore_signal(barrier, inc=1, device_id=(my_x + step_x, my_y + step_y), device_id_type=MESH)
        peers = peers + there.astype(i32)
    for hop in range(1, ny):
        pl.semaphore_signal(barrier, inc=1, device_id=(my_x, lax.rem(my_y + hop, ny)), device_id_type=MESH)
    for hop in range(1, nx):
        pl.semaphore_signal(barrier, inc=1, device_id=(lax.rem(my_x + hop, nx), my_y), device_id_type=MESH)

    def opposite(index):
        return index ^ 1 if index < 4 else 11 - index

    def outgoing(index, slot):
        step_x, step_y, _ = sides[index]
        if index < 2:
            src, dst = xpack.at[slot, index], xslot.at[slot, 1 - index]
        elif index < 4:
            src, dst = ypack.at[slot, index - 2], yslot.at[slot, 3 - index, pl.ds(2 * 8, rows * 8)]
        else:
            side = 0 if step_y < 0 else 1
            start = 0 if step_x < 0 else rows - 2
            land = rows + 2 if step_x < 0 else 0
            src = ypack.at[slot, side, pl.ds(start * 8, 16)]
            dst = yslot.at[slot, 1 - side, pl.ds(land * 8, 16)]
        return pltpu.make_async_remote_copy(
            src_ref=src, dst_ref=dst, send_sem=send_sem.at[slot, index], recv_sem=recv_sem.at[slot, opposite(index)],
            device_id=(my_x + step_x, my_y + step_y), device_id_type=MESH,
        )

    def outgoing_mask(index):
        step_x, step_y, _ = sides[index]
        if index < 2:
            pairs = [(mxpack.at[index], mxslot.at[1 - index])]
        elif index < 4:
            pairs = [
                (mypack.at[index - 2], myslot.at[3 - index, pl.ds(2 * 8, rows * 8)]),
                (my3pack.at[index - 2], my3slot.at[3 - index]),
            ]
        else:
            side = 0 if step_y < 0 else 1
            start = 0 if step_x < 0 else rows - 2
            land = rows + 2 if step_x < 0 else 0
            pairs = [(mypack.at[side, pl.ds(start * 8, 16)], myslot.at[1 - side, pl.ds(land * 8, 16)])]
        return [
            pltpu.make_async_remote_copy(
                src_ref=src, dst_ref=dst, send_sem=msend_sem.at[part, index],
                recv_sem=mrecv_sem.at[part, opposite(index)],
                device_id=(my_x + step_x, my_y + step_y), device_id_type=MESH,
            )
            for part, (src, dst) in enumerate(pairs)
        ]

    ORDER = (4, 5, 6, 7, 2, 3, 0, 1)

    def column(at):
        return pl.ds(at, rows, stride=cols)

    def spread(at):
        return pl.ds(at, rows, stride=8)

    def pack(source, slot):
        for side in range(2):
            for layer in (1, 2, 3):
                at = layer - 1 if side == 0 else cols - layer
                for c in range(3) if layer < 3 else (1,):
                    e = 3 * (layer - 1) + (c if layer < 3 else 0)
                    ypack[slot, side, spread(e), :] = source[c, column(at), :]
        for index in ORDER[:6]:
            @pl.when(sides[index][2])
            def _():
                outgoing(index, slot).start()
        for side in range(2):
            for layer in (1, 2, 3):
                at = layer - 1 if side == 0 else rows - layer
                for c in range(3) if layer < 3 else (0,):
                    e = 3 * (layer - 1) + c
                    xpack[slot, side, pl.ds(e * cols, cols), :] = source[c, pl.ds(at * cols, cols), :]
        for index in ORDER[6:]:
            @pl.when(sides[index][2])
            def _():
                outgoing(index, slot).start()

    def arrived(index, slot):
        outgoing(index, slot).wait_send()
        outgoing(opposite(index), slot).wait_recv()

    pad[...] = jnp.zeros_like(pad)
    mask_pad[...] = jnp.full_like(mask_pad, -1)
    diagonal[...] = jnp.zeros_like(diagonal)
    for state in (xg, xw, yg, yw, xr, ypack, acc):
        state[...] = jnp.zeros_like(state)
    for state in (mxr, myr, mx3, my3, mypack):
        state[...] = jnp.full_like(state, -1)
    ab[...] = jnp.where(lax.broadcasted_iota(i32, ab.shape, 0) == 0, 1.0, 0.0).astype(f32)
    place = lax.broadcasted_iota(i32, (1, depth), 1)
    fetches[0].wait()
    for word in range(4):
        for r in range(rows):
            mask_pad[word, 3 + r, pl.ds(EDGE, cols), :] = mask[word, pl.ds(r * cols, cols), :]

    for along in range(-3, 4):
        for word in range(4):
            mask_shifted[word] = mask_pad[word, :, pl.ds(EDGE + along, cols), :].reshape(-1, depth)
        for upward in range(-3, 4):
            across_all = reach(along, upward)
            if not across_all:
                continue
            inside = (place + upward >= 0) & (place + upward < depth)
            for low in range(0, rows, 4):
                here = pl.ds(low * cols, 4 * cols)
                moments = [None, None, None]
                for across in across_all:
                    word, bit, mirror_word, mirror_bit, weight = bond((across, along, upward))
                    own = mask[word, here] & bit
                    far = mask_shifted[mirror_word, pl.ds((3 + low + across) * cols, 4 * cols)] & mirror_bit
                    far = rolled(jnp.where(far == 0, f32(weight), f32(0.0)), upward)
                    one = jnp.where((own == 0) & inside, far, f32(0.0))
                    weights[NUMBER[(across, along, upward)], here] = one
                    for power in range(3):
                        scale = across**power
                        if scale:
                            moments[power] = add(moments[power], scaled(scale, one))
                for slot, (power, scale) in enumerate((
                    (2, 1), (1, along), (1, upward), (0, along * along), (0, along * upward), (0, upward * upward),
                )):
                    if scale and moments[power] is not None:
                        diagonal[slot, here] += scaled(scale, moments[power])

    for side in range(2):
        for layer in (1, 2):
            at = layer - 1 if side == 0 else cols - layer
            for word in range(4):
                mypack[side, spread(4 * (layer - 1) + word), :] = mask[word, column(at), :]
            at = layer - 1 if side == 0 else rows - layer
            for word in range(4):
                e = 4 * (layer - 1) + word
                mxpack[side, pl.ds(e * cols, cols), :] = mask[word, pl.ds(at * cols, cols), :]
        sign = 1 if side == 0 else -1
        word = bond((0, 3 * sign, 0))[2]
        my3pack[side] = mask[word, column(2 if side == 0 else cols - 3), :]
        word = bond((3 * sign, 0, 0))[2]
        mxpack[side, pl.ds(8 * cols, cols), :] = mask[word, pl.ds((2 if side == 0 else rows - 3) * cols, cols), :]

    pl.semaphore_wait(barrier, peers)
    for hop in range(1, ny):
        pl.semaphore_signal(ready, inc=1, device_id=(my_x, lax.rem(my_y + hop, ny)), device_id_type=MESH)
    for index in ORDER:
        @pl.when(sides[index][2])
        def _():
            for copy in outgoing_mask(index):
                copy.start()
    fetches[1].wait()
    pack(field, 0)
    fetches[2].wait()
    pack(speed, 1)

    middle = (slice(None), pl.ds(3, rows), pl.ds(EDGE, cols), slice(None))

    def set_pad(c, value):
        pad[c, pl.ds(3, rows), pl.ds(EDGE, cols), :] = value.reshape(rows, cols, depth)

    for c in range(3):
        set_pad(c, field[c])

    def face_weights(side):
        sign = -1 if side == 0 else 1
        for axis in (0, 1):
            terms = {}
            for layer, r in PLANES + LONG:
                for p, c in crossing(layer, r) if (layer, r) in PLANES else [(0, 0)]:
                    out = sign * (layer + r)
                    offset = (out, p, c) if axis == 0 else (p, out, c)
                    word, bit, mirror_word, mirror_bit, weight = bond(offset)
                    if axis == 0:
                        at = r if side == 0 else rows - 1 - r
                        own = mask[word, pl.ds(at * cols, cols), :]
                        if layer == 3:
                            far = mx3[side]
                        else:
                            far = mxr[side, c + 2, 4 * (layer - 1) + mirror_word, pl.ds(EDGE + p, cols), :]
                    else:
                        at = r if side == 0 else cols - 1 - r
                        own = mask[word, column(at), :]
                        if layer == 3:
                            far = my3[side]
                        else:
                            far = myr[side, c + 2, spread((2 + p) * 8 + 4 * (layer - 1) + mirror_word), :]
                    one = jnp.where(((own & bit) | (far & mirror_bit)) == 0, f32(weight), f32(0.0))
                    if axis == 0:
                        wx[side, FACE[layer, r, p, c]] = one
                    else:
                        wy[side, FACE[layer, r, p, c]] = one
                    slot = 0
                    for i in range(3):
                        for j in range(i, 3):
                            scale = offset[i] * offset[j]
                            if scale:
                                key = (r, slot)
                                terms[key] = add(terms.get(key), scaled(scale, one))
                            slot += 1
            for (r, slot), term in terms.items():
                if axis == 0:
                    at = r if side == 0 else rows - 1 - r
                    diagonal[slot, pl.ds(at * cols, cols), :] += term
                else:
                    at = r if side == 0 else cols - 1 - r
                    diagonal[slot, column(at), :] += term

    def take_masks():
        for index in range(8):
            step_x, step_y, there = sides[index]

            @pl.when(there)
            def _():
                for copy in outgoing_mask(index):
                    copy.wait_send()
                for copy in outgoing_mask(opposite(index)):
                    copy.wait_recv()
                for upward in range(-2, 3):
                    inside = (place + upward >= 0) & (place + upward < depth)
                    if index < 2:
                        words = mxslot[index, pl.ds(0, 8 * cols), :]
                    elif index < 4:
                        first, size = 2 * 8, rows * 8
                        words = myslot[index - 2, pl.ds(first, size), :]
                    else:
                        first, size = (0 if step_x < 0 else (rows + 2) * 8), 16
                        words = myslot[0 if step_y < 0 else 1, pl.ds(first, size), :]
                    if upward:
                        words = jnp.where(inside, rolled(words, upward), -1)
                    if index < 2:
                        mxr[index, upward + 2, :, pl.ds(EDGE, cols), :] = words.reshape(8, cols, depth)
                    else:
                        myr[0 if step_y < 0 else 1, upward + 2, pl.ds(first, size), :] = words
                if index < 2:
                    mx3[index] = mxslot[index, pl.ds(8 * cols, cols), :]
                elif index < 4:
                    my3[index - 2] = my3slot[index - 2]
        for side in range(2):
            face_weights(side)

    def own_forces():
        turn = 0
        for low in range(0, rows, 4):
            for c in range(3):
                force[c, pl.ds(low * cols, 4 * cols)] = jnp.zeros((4 * cols, depth), f32)
        for along in range(-3, 4):
            for c in range(3):
                shifted[c] = pad[c, :, pl.ds(EDGE + along, cols), :].reshape(-1, depth)
            for upward in range(-3, 4):
                across_all = reach(along, upward)
                if not across_all:
                    continue
                turn = 1 - turn
                most = max(across_all)
                span = pl.ds(3 * cols, rows * cols)
                if along or upward:
                    mix = None
                    for scale, c in ((along, 1), (upward, 2)):
                        if scale:
                            mix = add(mix, scaled(scale, shifted[c, span]))
                    mixed[turn, span] = rolled(mix, upward)
                if most:
                    plain[turn, span] = rolled(shifted[0, span], upward)
                for low in range(0, rows, 4):
                    here = pl.ds(low * cols, 4 * cols)
                    whole = None
                    lean = None

                    def stretch(across):
                        at = pl.ds((3 + low + across) * cols, 4 * cols)
                        value = mixed[turn, at] if along or upward else None
                        if across:
                            term = float(across) * plain[turn, at]
                            value = term if value is None else value + term
                        return weights[NUMBER[(across, along, upward)], here] * value

                    for across in [a for a in across_all if a >= 0]:
                        if across == 0:
                            whole = stretch(0)
                            continue
                        up, down = stretch(across), stretch(-across)
                        both = up + down
                        whole = both if whole is None else whole + both
                        lean = add(lean, scaled(across, up - down))
                    if lean is not None:
                        force[0, here] += lean
                    if along:
                        force[1, here] += float(along) * whole
                    if upward:
                        force[2, here] += float(upward) * whole

    def diagonal_forces():
        for low in range(0, rows, 4):
            here = pl.ds(low * cols, 4 * cols)
            u = [pad[c, pl.ds(3 + low, 4), pl.ds(EDGE, cols), :].reshape(4 * cols, depth) for c in range(3)]
            d = [diagonal[slot, here] for slot in range(6)]
            force[0, here] -= d[0] * u[0] + d[1] * u[1] + d[2] * u[2]
            force[1, here] -= d[1] * u[0] + d[3] * u[1] + d[4] * u[2]
            force[2, here] -= d[2] * u[0] + d[4] * u[1] + d[5] * u[2]

    def face_forces(axis, side):
        sign = -1 if side == 0 else 1
        normal, tangent = (0, 1) if axis == 0 else (1, 0)
        result = {}
        for layer in (1, 2):
            inner = [r for one, r in PLANES if one == layer]
            wide = {}
            for c in range(-2, 3):
                sums = {}
                for p in range(-2, 3):
                    targets = [r for r in inner if (layer, r, p, c) in FACE]
                    if not targets:
                        continue

                    def near(component):
                        e = 3 * (layer - 1) + component
                        if axis == 0:
                            return xr[side, c + 2, e, pl.ds(EDGE + p, cols), :]
                        return yr[side, c + 2, spread((2 + p) * 8 + e), :]

                    out = near(normal)
                    base = None
                    if p:
                        base = scaled(p, near(tangent))
                    if c:
                        base = add(base, scaled(c, near(2)))
                    for r in targets:
                        value = scaled(sign * (layer + r), out)
                        if base is not None:
                            value = value + base
                        one = (wx if axis == 0 else wy)[side, FACE[layer, r, p, c]] * value
                        sums[r, 0] = add(sums.get((r, 0)), one)
                        if p:
                            sums[r, 1] = add(sums.get((r, 1)), scaled(p, one))
                for r in inner:
                    if (r, 0) not in sums:
                        continue
                    wide[r, normal] = add(wide.get((r, normal)), sums[r, 0])
                    if (r, 1) in sums:
                        wide[r, tangent] = add(wide.get((r, tangent)), sums[r, 1])
                    if c:
                        wide[r, 2] = add(wide.get((r, 2)), scaled(c, sums[r, 0]))
            for r in inner:
                wide[r, normal] = scaled(sign * (layer + r), wide[r, normal])
                for component in range(3):
                    result[r, component] = add(result.get((r, component)), wide[r, component])
        for layer, r in LONG:
            e = 6 if layer == 3 else 3 * (layer - 1) + normal
            if axis == 0:
                out = xg[side, pl.ds(e * cols, cols), :]
            else:
                out = yg[side, spread(2 * 8 + e), :]
            one = 9.0 * ((wx if axis == 0 else wy)[side, FACE[layer, r, 0, 0]] * out)
            result[r, normal] = add(result.get((r, normal)), one)
        for (r, component), term in result.items():
            if axis == 0:
                at = r if side == 0 else rows - 1 - r
                force[component, pl.ds(at * cols, cols), :] += term
            else:
                at = r if side == 0 else cols - 1 - r
                force[component, column(at), :] += term

    me = my_x * ny + my_y

    def dot(first, second):
        whole = None
        for c in range(3):
            whole = add(whole, jnp.sum((first[c] * second[c]).reshape(-1, 8, depth), axis=0))
        return whole

    def send_sums(slot):
        line = jnp.zeros((1, depth), f32)
        for which in range(6):
            one = jnp.sum(jnp.sum(acc[which], axis=0, keepdims=True), axis=1, keepdims=True)
            line = jnp.where(place == which, one, line)
        sums_out[slot] = line

        def send(r, carry):
            target = lax.rem(me + 1 + r, devices)
            pltpu.make_async_remote_copy(
                src_ref=sums_out.at[slot], dst_ref=sums_in.at[slot, r],
                send_sem=sum_send_sem.at[slot], recv_sem=sum_recv_sem.at[slot],
                device_id=(target // ny, lax.rem(target, ny)), device_id_type=MESH,
            ).start()
            return carry

        lax.fori_loop(0, devices - 1, send, 0)

    def take_sums(slot):
        whole = sums_in.at[slot]
        pltpu.make_async_copy(whole, whole, sum_send_sem.at[slot]).wait()
        pltpu.make_async_copy(whole, whole, sum_recv_sem.at[slot]).wait()
        line = jnp.sum(sums_in[slot], axis=0) + sums_out[slot]
        vv, vg, gg, vw, wg, gh = [
            jnp.sum(jnp.where(place == which, line, 0.0), axis=1, keepdims=True) for which in range(6)
        ]
        alpha, beta = ab[0:1, 0:1], ab[1:2, 0:1]
        kinetic = alpha * alpha * vv + 2.0 * alpha * beta * vg + beta * beta * gg
        rayleigh = -(alpha * alpha * vw + 2.0 * alpha * beta * wg + beta * beta * gh)
        damping = 2.0 * jnp.sqrt(rayleigh / count / (fictive_mass * (kinetic / count + epsilon)))
        alpha = (2.0 - damping) / (2.0 + damping)
        beta = 2.0 / (fictive_mass * (2.0 + damping))
        ab[0:1, :] = jnp.broadcast_to(alpha, (1, depth))
        ab[1:2, :] = jnp.broadcast_to(beta, (1, depth))
        return alpha, beta

    def step(turn, carry):
        own_forces()

        @pl.when(turn == 0)
        def _():
            take_masks()

        diagonal_forces()

        slot = jnp.where(turn < 3, turn, lax.rem(turn + 1, SLOTS))
        early = turn < 3
        alpha = jnp.where(early, 0.0, ab[0:1, :])
        beta = jnp.where(early, 1.0, ab[1:2, :])
        keep = jnp.where(early, 0.0, jnp.ones((1, depth), f32))

        @pl.when(turn == 3)
        def _():
            for index in range(8):
                step_x, step_y, there = sides[index]

                @pl.when(there)
                def _():
                    arrived(index, 3)
                    if index < 2:
                        xw[index] = xslot[3, index]
                    else:
                        side = 0 if step_y < 0 else 1
                        here = pl.ds(16, rows * 8) if index < 4 else pl.ds(0 if step_x < 0 else (rows + 2) * 8, 16)
                        yw[side, here] = yslot[3, side, here]

        for index in (0, 1):
            @pl.when(sides[index][2])
            def _():
                arrived(index, slot)
                fresh = alpha * xw[index] + beta * xslot[slot, index]
                xw[index] = fresh
                fresh = keep * xg[index] + fresh
                xg[index] = fresh
                for upward in range(-2, 3):
                    xr[index, upward + 2, :, pl.ds(EDGE, cols), :] = rolled(
                        fresh[: 6 * cols], upward).reshape(6, cols, depth)
        for side in range(2):
            face_forces(0, side)
        for index in range(2, 8):
            step_x, step_y, there = sides[index]

            @pl.when(there)
            def _():
                arrived(index, slot)
                side = 0 if step_y < 0 else 1
                here = pl.ds(16, rows * 8) if index < 4 else pl.ds(0 if step_x < 0 else (rows + 2) * 8, 16)
                fresh = alpha * yw[side, here] + beta * yslot[slot, side, here]
                yw[side, here] = fresh
                yg[side, here] = keep * yg[side, here] + fresh
        for side in range(2):
            for upward in range(-2, 3):
                yr[side, upward + 2] = rolled(yg[side], upward)
        for side in range(2):
            face_forces(1, side)

        @pl.when(turn == 0)
        def _():
            fetches[3].wait()
            fetches[4].wait()
            for c in range(3):
                whole = force[c] + flags[...].astype(f32) * load[c]
                force[c] = whole
                total[c] = whole

        @pl.when(turn < ITERS)
        def _():
            pack(force, lax.rem(turn + 2, SLOTS))

        @pl.when(turn == 0)
        def _():
            for c in range(3):
                set_pad(c, speed[c])

        @pl.when(turn == 1)
        def _():
            for c in range(3):
                change[c] = force[c]
                set_pad(c, total[c])
            acc[0] = dot(speed, speed)
            acc[1] = dot(speed, total)
            acc[2] = dot(total, total)
            acc[3] = dot(speed, force)
            acc[4] = dot(force, total)
            pl.semaphore_wait(ready, ny - 1)
            send_sums(0)

        @pl.when(turn >= 2)
        def _():
            acc[5] = dot(total, force)
            send_sums(lax.rem(turn - 1, SLOTS))
            alpha, beta = take_sums(lax.rem(turn - 2, SLOTS))
            sums = [None] * 5
            for c in range(3):
                w = alpha * change[c] + beta * force[c]
                v = alpha * speed[c] + beta * total[c]
                g = total[c] + w
                change[c] = w
                speed[c] = v
                total[c] = g
                field[c] = field[c] + v
                set_pad(c, g)
                for which, (a, b) in enumerate(((v, v), (v, g), (g, g), (v, w), (w, g))):
                    sums[which] = add(sums[which], jnp.sum((a * b).reshape(-1, 8, depth), axis=0))
            for which in range(5):
                acc[which] = sums[which]

        return carry

    lax.fori_loop(0, ITERS + 1, step, 0)
    alpha, beta = take_sums((ITERS - 1) % SLOTS)
    for c in range(3):
        v = alpha * speed[c] + beta * total[c]
        speed[c] = v
        field[c] = field[c] + v


def on_device(nx, ny, disp, vel, load, flags, mask_bits):
    parts, rows, cols, depth = disp.shape
    words = mask_bits.shape[0]
    cells = rows * cols
    f32, i32 = jnp.float32, jnp.int32
    vmem, dma = pltpu.VMEM, pltpu.SemaphoreType.DMA
    wide = cols + 2 * EDGE
    flat = (parts, cells, depth)
    tall = (rows + 6) * cols
    ring = (rows + 4) * 8
    scratch = [
        vmem(flat, f32),
        vmem((cells, depth), i32),
        vmem((words, cells, depth), i32),
        vmem((len(TABLE), cells, depth), f32),
        vmem((6, cells, depth), f32),
        vmem((parts, rows + 6, wide, depth), f32),
        vmem((words, rows + 6, wide, depth), i32),
        vmem((parts, tall, depth), f32),
        vmem((words, tall, depth), i32),
        vmem((2, tall, depth), f32),
        vmem((2, tall, depth), f32),
        vmem(flat, f32),
        vmem(flat, f32),
        vmem(flat, f32),
        vmem((2, len(FACE), cols, depth), f32),
        vmem((2, len(FACE), rows, depth), f32),
        vmem((2, 7 * cols, depth), f32),
        vmem((2, 7 * cols, depth), f32),
        vmem((2, ring, depth), f32),
        vmem((2, ring, depth), f32),
        vmem((2, 5, 6, wide, depth), f32),
        vmem((2, 5, ring, depth), f32),
        vmem((2, 5, 8, wide, depth), i32),
        vmem((2, 5, ring, depth), i32),
        vmem((2, cols, depth), i32),
        vmem((2, rows, depth), i32),
        vmem((SLOTS, 2, 7 * cols, depth), f32),
        vmem((SLOTS, 2, rows * 8, depth), f32),
        vmem((SLOTS, 2, 7 * cols, depth), f32),
        vmem((SLOTS, 2, ring, depth), f32),
        vmem((2, 9 * cols, depth), i32),
        vmem((2, rows * 8, depth), i32),
        vmem((2, rows, depth), i32),
        vmem((2, 9 * cols, depth), i32),
        vmem((2, ring, depth), i32),
        vmem((2, rows, depth), i32),
        vmem((6, 8, depth), f32),
        vmem((8, depth), f32),
        vmem((SLOTS, 1, depth), f32),
        vmem((SLOTS, nx * ny - 1, 1, depth), f32),
        dma((5,)),
        dma((SLOTS, 8)),
        dma((SLOTS, 8)),
        dma((2, 8)),
        dma((2, 8)),
        dma((SLOTS,)),
        dma((SLOTS,)),
        pltpu.SemaphoreType.REGULAR,
    ]
    outs = pl.pallas_call(
        functools.partial(kernel, nx, ny),
        out_shape=[jax.ShapeDtypeStruct(flat, f32)] * 2,
        in_specs=[pl.BlockSpec(memory_space=pltpu.HBM)] * 5,
        out_specs=[pl.BlockSpec(memory_space=pltpu.VMEM)] * 2,
        scratch_shapes=scratch,
        compiler_params=pltpu.CompilerParams(
            has_side_effects=True, collective_id=0, vmem_limit_bytes=48 * 1024 * 1024),
    )(disp.reshape(flat), vel.reshape(flat), load.reshape(flat), flags.reshape(cells, depth),
      mask_bits.reshape(words, cells, depth))
    return tuple(out.reshape(disp.shape) for out in outs)


def solution(mesh):
    cells = P(None, "gx", "gy", None)
    return jax.shard_map(
        functools.partial(on_device, mesh.shape["gx"], mesh.shape["gy"]),
        mesh=mesh,
        in_specs=(cells, cells, cells, P("gx", "gy", None), cells),
        out_specs=(cells, cells),
        check_vma=False,
    )
```

```python
import functools
import math

import jax
import jax.numpy as jnp
from jax import lax
from jax.experimental import pallas as pl
from jax.experimental.pallas import tpu as pltpu
from jax.sharding import PartitionSpec as P

ITERS = 8
MESH = pl.DeviceIdType.MESH

fictive_mass = 64.0
epsilon = 1e-06

EDGE = 8
SLOTS = 4
EARLY = 2


def neighbour_table():
    table = []
    for across in range(-3, 4):
        for along in range(-3, 4):
            for upward in range(-3, 4):
                length = across * across + along * along + upward * upward
                if 0 < length <= 9:
                    table.append((across, along, upward))
    return table


TABLE = neighbour_table()
NUMBER = {offset: number for number, offset in enumerate(TABLE)}

PLANES = [(1, 0), (1, 1), (2, 0)]
LONG = [(1, 2), (2, 1), (3, 0)]


def reach(along, upward):
    return [a for a in range(-3, 4) if (a, along, upward) in NUMBER]


def crossing(layer, r):
    far = layer + r
    return [(p, c) for c in range(-2, 3) for p in range(-2, 3) if far * far + p * p + c * c <= 9]


SLOT = {(0, 0): 0, (0, 1): 1, (0, 2): 2, (1, 1): 3, (1, 2): 4, (2, 2): 5}
FACE = {}
for plane in PLANES:
    for offset in crossing(*plane):
        FACE[plane + offset] = len(FACE)
for plane in LONG:
    FACE[plane + (0, 0)] = len(FACE)


def bond(offset):
    number = NUMBER[offset]
    word, bit = divmod(number, 31)
    mirror_word, mirror_bit = divmod(121 - number, 31)
    length = float(sum(part * part for part in offset))
    return word, 1 << bit, mirror_word, 1 << mirror_bit, 1.0 / (length * math.sqrt(length))


def rolled(cells, upward):
    depth = cells.shape[-1]
    if upward == 0:
        return cells
    return pltpu.roll(cells, (-upward) % depth, cells.ndim - 1)


def add(total, term):
    return term if total is None else total + term


def scaled(scale, value):
    return value if scale == 1 else float(scale) * value


def kernel(
    nx, ny,
    disp_in, vel_in, load_in, flags_in, mask_in,
    field, speed,
    load, flags, mask,
    weights, diagonal, pad, mask_pad, shifted, mask_shifted, mixed, plain, force, total, change,
    wx, wy, xg, xw, yg, yw, xr, yr, mxr, myr, mx3, my3,
    xpack, ypack, xslot, yslot, mxpack, mypack, my3pack, mxslot, myslot, my3slot,
    acc, ab, sums_out, sums_in,
    local_sem, send_sem, recv_sem, msend_sem, mrecv_sem, sum_send_sem, sum_recv_sem, ready,
):
    depth = flags.shape[-1]
    cells = flags.shape[0]
    rows = pad.shape[1] - 6
    cols = cells // rows
    count = 3.0 * rows * nx * cols * ny * depth
    my_x = lax.axis_index("gx")
    my_y = lax.axis_index("gy")
    f32, i32 = jnp.float32, jnp.int32

    fetches = [
        pltpu.make_async_copy(src, dst, local_sem.at[index])
        for index, (src, dst) in enumerate((
            (mask_in, mask), (disp_in, field), (vel_in, speed), (load_in, load), (flags_in, flags),
        ))
    ]
    for fetch in fetches:
        fetch.start()

    sides = []
    for step_x, step_y in ((-1, 0), (1, 0), (0, -1), (0, 1), (-1, -1), (-1, 1), (1, -1), (1, 1)):
        there = None
        for step, mine, size in ((step_x, my_x, nx), (step_y, my_y, ny)):
            if step:
                near = mine > 0 if step < 0 else mine < size - 1
                there = near if there is None else there & near
        sides.append((step_x, step_y, there))

    barrier = pltpu.get_barrier_semaphore()
    peers = nx + ny - 2
    for step_x, step_y, there in sides[4:]:
        @pl.when(there)
        def _():
            pl.semaphore_signal(barrier, inc=1, device_id=(my_x + step_x, my_y + step_y), device_id_type=MESH)
        peers = peers + there.astype(i32)
    for hop in range(1, ny):
        pl.semaphore_signal(barrier, inc=1, device_id=(my_x, lax.rem(my_y + hop, ny)), device_id_type=MESH)
    for hop in range(1, nx):
        pl.semaphore_signal(barrier, inc=1, device_id=(lax.rem(my_x + hop, nx), my_y), device_id_type=MESH)

    def opposite(index):
        return index ^ 1 if index < 4 else 11 - index

    def outgoing(index, slot):
        step_x, step_y, _ = sides[index]
        if index < 2:
            src, dst = xpack.at[slot, index], xslot.at[slot, 1 - index]
        elif index < 4:
            src, dst = ypack.at[slot, index - 2], yslot.at[slot, 3 - index, pl.ds(2 * 8, rows * 8)]
        else:
            side = 0 if step_y < 0 else 1
            start = 0 if step_x < 0 else rows - 2
            land = rows + 2 if step_x < 0 else 0
            src = ypack.at[slot, side, pl.ds(start * 8, 16)]
            dst = yslot.at[slot, 1 - side, pl.ds(land * 8, 16)]
        return pltpu.make_async_remote_copy(
            src_ref=src, dst_ref=dst, send_sem=send_sem.at[slot, index], recv_sem=recv_sem.at[slot, opposite(index)],
            device_id=(my_x + step_x, my_y + step_y), device_id_type=MESH,
        )

    def outgoing_mask(index):
        step_x, step_y, _ = sides[index]
        if index < 2:
            pairs = [(mxpack.at[index], mxslot.at[1 - index])]
        elif index < 4:
            pairs = [
                (mypack.at[index - 2], myslot.at[3 - index, pl.ds(2 * 8, rows * 8)]),
                (my3pack.at[index - 2], my3slot.at[3 - index]),
            ]
        else:
            side = 0 if step_y < 0 else 1
            start = 0 if step_x < 0 else rows - 2
            land = rows + 2 if step_x < 0 else 0
            pairs = [(mypack.at[side, pl.ds(start * 8, 16)], myslot.at[1 - side, pl.ds(land * 8, 16)])]
        return [
            pltpu.make_async_remote_copy(
                src_ref=src, dst_ref=dst, send_sem=msend_sem.at[part, index],
                recv_sem=mrecv_sem.at[part, opposite(index)],
                device_id=(my_x + step_x, my_y + step_y), device_id_type=MESH,
            )
            for part, (src, dst) in enumerate(pairs)
        ]

    ORDER = (4, 5, 6, 7, 2, 3, 0, 1)

    def column(at):
        return pl.ds(at, rows, stride=cols)

    def spread(at):
        return pl.ds(at, rows, stride=8)

    def pack(source, slot):
        for side in range(2):
            for layer in (1, 2, 3):
                at = layer - 1 if side == 0 else cols - layer
                for c in range(3) if layer < 3 else (1,):
                    e = 3 * (layer - 1) + (c if layer < 3 else 0)
                    ypack[slot, side, spread(e), :] = source[c, column(at), :]
        for index in ORDER[:6]:
            @pl.when(sides[index][2])
            def _():
                outgoing(index, slot).start()
        for side in range(2):
            for layer in (1, 2, 3):
                at = layer - 1 if side == 0 else rows - layer
                for c in range(3) if layer < 3 else (0,):
                    e = 3 * (layer - 1) + c
                    xpack[slot, side, pl.ds(e * cols, cols), :] = source[c, pl.ds(at * cols, cols), :]
        for index in ORDER[6:]:
            @pl.when(sides[index][2])
            def _():
                outgoing(index, slot).start()

    def arrived(index, slot):
        outgoing(index, slot).wait_send()
        outgoing(opposite(index), slot).wait_recv()

    pad[...] = jnp.zeros_like(pad)
    mask_pad[...] = jnp.full_like(mask_pad, -1)
    diagonal[...] = jnp.zeros_like(diagonal)
    for state in (xg, xw, yg, yw, xr, ypack, acc):
        state[...] = jnp.zeros_like(state)
    for state in (mxr, myr, mx3, my3, mypack):
        state[...] = jnp.full_like(state, -1)
    ab[...] = jnp.where(lax.broadcasted_iota(i32, ab.shape, 0) == 0, 1.0, 0.0).astype(f32)
    place = lax.broadcasted_iota(i32, (1, depth), 1)
    fetches[0].wait()
    for word in range(4):
        for r in range(rows):
            mask_pad[word, 3 + r, pl.ds(EDGE, cols), :] = mask[word, pl.ds(r * cols, cols), :]

    for side in range(2):
        for layer in (1, 2):
            at = layer - 1 if side == 0 else cols - layer
            for word in range(4):
                mypack[side, spread(4 * (layer - 1) + word), :] = mask[word, column(at), :]
            at = layer - 1 if side == 0 else rows - layer
            for word in range(4):
                e = 4 * (layer - 1) + word
                mxpack[side, pl.ds(e * cols, cols), :] = mask[word, pl.ds(at * cols, cols), :]
        sign = 1 if side == 0 else -1
        word = bond((0, 3 * sign, 0))[2]
        my3pack[side] = mask[word, column(2 if side == 0 else cols - 3), :]
        word = bond((3 * sign, 0, 0))[2]
        mxpack[side, pl.ds(8 * cols, cols), :] = mask[word, pl.ds((2 if side == 0 else rows - 3) * cols, cols), :]

    def own_weights(along):
        for word in range(4):
            mask_shifted[word] = mask_pad[word, :, pl.ds(EDGE + along, cols), :].reshape(-1, depth)
        for upward in range(-3, 4):
            across_all = reach(along, upward)
            if not across_all:
                continue
            inside = (place + upward >= 0) & (place + upward < depth)
            for low in range(0, rows, 4):
                here = pl.ds(low * cols, 4 * cols)
                moments = [None, None, None]
                for across in across_all:
                    word, bit, mirror_word, mirror_bit, weight = bond((across, along, upward))
                    own = mask[word, here] & bit
                    far = mask_shifted[mirror_word, pl.ds((3 + low + across) * cols, 4 * cols)] & mirror_bit
                    far = rolled(jnp.where(far == 0, f32(weight), f32(0.0)), upward)
                    one = jnp.where((own == 0) & inside, far, f32(0.0))
                    weights[NUMBER[(across, along, upward)], here] = one
                    for power in range(3):
                        scale = across**power
                        if scale:
                            moments[power] = add(moments[power], scaled(scale, one))
                for slot, (power, scale) in enumerate((
                    (2, 1), (1, along), (1, upward), (0, along * along), (0, along * upward), (0, upward * upward),
                )):
                    if scale and moments[power] is not None:
                        diagonal[slot, here] += scaled(scale, moments[power])

    for along in range(-3, -3 + EARLY):
        own_weights(along)
    pl.semaphore_wait(barrier, peers)
    for hop in range(1, ny):
        pl.semaphore_signal(ready, inc=1, device_id=(my_x, lax.rem(my_y + hop, ny)), device_id_type=MESH)
    for index in ORDER:
        @pl.when(sides[index][2])
        def _():
            for copy in outgoing_mask(index):
                copy.start()
    fetches[1].wait()
    pack(field, 0)
    for along in range(-3 + EARLY, 4):
        own_weights(along)

    middle = (slice(None), pl.ds(3, rows), pl.ds(EDGE, cols), slice(None))

    def set_pad(c, value):
        pad[c, pl.ds(3, rows), pl.ds(EDGE, cols), :] = value.reshape(rows, cols, depth)

    for c in range(3):
        set_pad(c, field[c])

    def face_weights(side):
        sign = -1 if side == 0 else 1
        for axis in (0, 1):
            terms, powers = {}, {}
            for layer, r in PLANES + LONG:
                for p, c in crossing(layer, r) if (layer, r) in PLANES else [(0, 0)]:
                    out = sign * (layer + r)
                    offset = (out, p, c) if axis == 0 else (p, out, c)
                    word, bit, mirror_word, mirror_bit, weight = bond(offset)
                    if axis == 0:
                        at = r if side == 0 else rows - 1 - r
                        own = mask[word, pl.ds(at * cols, cols), :]
                        if layer == 3:
                            far = mx3[side]
                        else:
                            far = mxr[side, c + 2, 4 * (layer - 1) + mirror_word, pl.ds(EDGE + p, cols), :]
                    else:
                        at = r if side == 0 else cols - 1 - r
                        own = mask[word, column(at), :]
                        if layer == 3:
                            far = my3[side]
                        else:
                            far = myr[side, c + 2, spread((2 + p) * 8 + 4 * (layer - 1) + mirror_word), :]
                    one = jnp.where(((own & bit) | (far & mirror_bit)) == 0, f32(weight), f32(0.0))
                    if axis == 0:
                        wx[side, FACE[layer, r, p, c]] = one
                    else:
                        wy[side, FACE[layer, r, p, c]] = one
                    for power in range(3):
                        if p**power:
                            key = (out, r, c, power)
                            powers[key] = add(powers.get(key), scaled(p**power, one))
            for (out, r, c, power), term in powers.items():
                for parts in ((0, 0), (0, 1), (0, 2), (1, 1), (1, 2), (2, 2)):
                    tangent = 1 - axis
                    if parts.count(tangent) != power:
                        continue
                    scale = out ** parts.count(axis) * c ** parts.count(2)
                    if scale:
                        key = (r, SLOT[parts])
                        terms[key] = add(terms.get(key), scaled(scale, term))
            for (r, slot), term in terms.items():
                if axis == 0:
                    at = r if side == 0 else rows - 1 - r
                    diagonal[slot, pl.ds(at * cols, cols), :] += term
                else:
                    at = r if side == 0 else cols - 1 - r
                    diagonal[slot, column(at), :] += term

    def take_masks():
        for index in range(8):
            step_x, step_y, there = sides[index]

            @pl.when(there)
            def _():
                for copy in outgoing_mask(index):
                    copy.wait_send()
                for copy in outgoing_mask(opposite(index)):
                    copy.wait_recv()
                for upward in range(-2, 3):
                    inside = (place + upward >= 0) & (place + upward < depth)
                    if index < 2:
                        words = mxslot[index, pl.ds(0, 8 * cols), :]
                    elif index < 4:
                        first, size = 2 * 8, rows * 8
                        words = myslot[index - 2, pl.ds(first, size), :]
                    else:
                        first, size = (0 if step_x < 0 else (rows + 2) * 8), 16
                        words = myslot[0 if step_y < 0 else 1, pl.ds(first, size), :]
                    if upward:
                        words = jnp.where(inside, rolled(words, upward), -1)
                    if index < 2:
                        mxr[index, upward + 2, :, pl.ds(EDGE, cols), :] = words.reshape(8, cols, depth)
                    else:
                        myr[0 if step_y < 0 else 1, upward + 2, pl.ds(first, size), :] = words
                if index < 2:
                    mx3[index] = mxslot[index, pl.ds(8 * cols, cols), :]
                elif index < 4:
                    my3[index - 2] = my3slot[index - 2]
        for side in range(2):
            face_weights(side)

    def own_forces():
        turn = 0
        for low in range(0, rows, 4):
            for c in range(3):
                force[c, pl.ds(low * cols, 4 * cols)] = jnp.zeros((4 * cols, depth), f32)
        for along in range(-3, 4):
            for c in range(3):
                shifted[c] = pad[c, :, pl.ds(EDGE + along, cols), :].reshape(-1, depth)
            for upward in range(-3, 4):
                across_all = reach(along, upward)
                if not across_all:
                    continue
                turn = 1 - turn
                most = max(across_all)
                span = pl.ds(3 * cols, rows * cols)
                if along or upward:
                    mix = None
                    for scale, c in ((along, 1), (upward, 2)):
                        if scale:
                            mix = add(mix, scaled(scale, shifted[c, span]))
                    mixed[turn, span] = rolled(mix, upward)
                if most:
                    plain[turn, span] = rolled(shifted[0, span], upward)
                for low in range(0, rows, 4):
                    here = pl.ds(low * cols, 4 * cols)
                    whole = None
                    lean = None

                    def stretch(across):
                        at = pl.ds((3 + low + across) * cols, 4 * cols)
                        value = mixed[turn, at] if along or upward else None
                        if across:
                            term = float(across) * plain[turn, at]
                            value = term if value is None else value + term
                        return weights[NUMBER[(across, along, upward)], here] * value

                    for across in [a for a in across_all if a >= 0]:
                        if across == 0:
                            whole = stretch(0)
                            continue
                        up, down = stretch(across), stretch(-across)
                        both = up + down
                        whole = both if whole is None else whole + both
                        lean = add(lean, scaled(across, up - down))
                    if lean is not None:
                        force[0, here] += lean
                    if along:
                        force[1, here] += float(along) * whole
                    if upward:
                        force[2, here] += float(upward) * whole

    def diagonal_forces():
        for low in range(0, rows, 4):
            here = pl.ds(low * cols, 4 * cols)
            u = [pad[c, pl.ds(3 + low, 4), pl.ds(EDGE, cols), :].reshape(4 * cols, depth) for c in range(3)]
            d = [diagonal[slot, here] for slot in range(6)]
            force[0, here] -= d[0] * u[0] + d[1] * u[1] + d[2] * u[2]
            force[1, here] -= d[1] * u[0] + d[3] * u[1] + d[4] * u[2]
            force[2, here] -= d[2] * u[0] + d[4] * u[1] + d[5] * u[2]

    def face_forces(axis, side, sign):
        normal, tangent = (0, 1) if axis == 0 else (1, 0)
        result = {}
        for layer in (1, 2):
            inner = [r for one, r in PLANES if one == layer]
            wide = {}
            for c in range(-2, 3):
                sums = {}
                for p in range(-2, 3):
                    targets = [r for r in inner if (layer, r, p, c) in FACE]
                    if not targets:
                        continue

                    def near(component):
                        e = 3 * (layer - 1) + component
                        if axis == 0:
                            return xr[side, c + 2, e, pl.ds(EDGE + p, cols), :]
                        return yr[side, c + 2, spread((2 + p) * 8 + e), :]

                    out = sign * near(normal)
                    base = None
                    if p:
                        base = scaled(p, near(tangent))
                    if c:
                        base = add(base, scaled(c, near(2)))
                    for r in targets:
                        value = scaled(layer + r, out)
                        if base is not None:
                            value = value + base
                        one = (wx if axis == 0 else wy)[side, FACE[layer, r, p, c]] * value
                        sums[r, 0] = add(sums.get((r, 0)), one)
                        if p:
                            sums[r, 1] = add(sums.get((r, 1)), scaled(p, one))
                for r in inner:
                    if (r, 0) not in sums:
                        continue
                    wide[r, normal] = add(wide.get((r, normal)), sums[r, 0])
                    if (r, 1) in sums:
                        wide[r, tangent] = add(wide.get((r, tangent)), sums[r, 1])
                    if c:
                        wide[r, 2] = add(wide.get((r, 2)), scaled(c, sums[r, 0]))
            for r in inner:
                wide[r, normal] = sign * scaled(layer + r, wide[r, normal])
                for component in range(3):
                    result[r, component] = add(result.get((r, component)), wide[r, component])
        for layer, r in LONG:
            e = 6 if layer == 3 else 3 * (layer - 1) + normal
            if axis == 0:
                out = xg[side, pl.ds(e * cols, cols), :]
            else:
                out = yg[side, spread(2 * 8 + e), :]
            one = 9.0 * ((wx if axis == 0 else wy)[side, FACE[layer, r, 0, 0]] * out)
            result[r, normal] = add(result.get((r, normal)), one)
        for (r, component), term in result.items():
            if axis == 0:
                at = r if side == 0 else rows - 1 - r
                force[component, pl.ds(at * cols, cols), :] += term
            else:
                at = jnp.where(side == 0, r, cols - 1 - r)
                force[component, column(at), :] += term

    hops = [(hop_x, hop_y) for hop_y in range(ny) for hop_x in range(nx) if hop_x or hop_y]
    hops.sort(key=lambda hop: (abs(2 * hop[1] - ny), abs(2 * hop[0] - nx)))

    def dot(first, second):
        whole = None
        for c in range(3):
            whole = add(whole, jnp.sum((first[c] * second[c]).reshape(-1, 8, depth), axis=0))
        return whole

    def send_sums(slot):
        line = jnp.zeros((1, depth), f32)
        for which in range(6):
            one = jnp.sum(jnp.sum(acc[which], axis=0, keepdims=True), axis=1, keepdims=True)
            line = jnp.where(place == which, one, line)
        sums_out[slot] = line

        for which, (hop_x, hop_y) in enumerate(hops):
            pltpu.make_async_remote_copy(
                src_ref=sums_out.at[slot], dst_ref=sums_in.at[slot, which],
                send_sem=sum_send_sem.at[slot], recv_sem=sum_recv_sem.at[slot],
                device_id=(lax.rem(my_x + hop_x, nx), lax.rem(my_y + hop_y, ny)), device_id_type=MESH,
            ).start()

    def take_sums(slot):
        whole = sums_in.at[slot]
        pltpu.make_async_copy(whole, whole, sum_send_sem.at[slot]).wait()
        pltpu.make_async_copy(whole, whole, sum_recv_sem.at[slot]).wait()
        line = jnp.sum(sums_in[slot], axis=0) + sums_out[slot]
        vv, vg, gg, vw, wg, gh = [
            jnp.sum(jnp.where(place == which, line, 0.0), axis=1, keepdims=True) for which in range(6)
        ]
        alpha, beta = ab[0:1, 0:1], ab[1:2, 0:1]
        kinetic = alpha * alpha * vv + 2.0 * alpha * beta * vg + beta * beta * gg
        rayleigh = -(alpha * alpha * vw + 2.0 * alpha * beta * wg + beta * beta * gh)
        damping = 2.0 * jnp.sqrt(rayleigh / count / (fictive_mass * (kinetic / count + epsilon)))
        alpha = (2.0 - damping) / (2.0 + damping)
        beta = 2.0 / (fictive_mass * (2.0 + damping))
        ab[0:1, :] = jnp.broadcast_to(alpha, (1, depth))
        ab[1:2, :] = jnp.broadcast_to(beta, (1, depth))
        return alpha, beta

    near_side = 1 - lax.rem(my_y, 2)

    def step(turn, carry):
        own_forces()

        @pl.when(turn == 0)
        def _():
            fetches[2].wait()
            pack(speed, 1)
            take_masks()

        diagonal_forces()

        slot = jnp.where(turn < 3, turn, lax.rem(turn + 1, SLOTS))
        early = turn < 3
        alpha = jnp.where(early, 0.0, ab[0:1, :])
        beta = jnp.where(early, 1.0, ab[1:2, :])
        keep = jnp.where(early, 0.0, jnp.ones((1, depth), f32))

        @pl.when(turn == 3)
        def _():
            for index in range(8):
                step_x, step_y, there = sides[index]

                @pl.when(there)
                def _():
                    arrived(index, 3)
                    if index < 2:
                        xw[index] = xslot[3, index]
                    else:
                        side = 0 if step_y < 0 else 1
                        here = pl.ds(16, rows * 8) if index < 4 else pl.ds(0 if step_x < 0 else (rows + 2) * 8, 16)
                        yw[side, here] = yslot[3, side, here]

        for index in (0, 1):
            @pl.when(sides[index][2])
            def _():
                arrived(index, slot)
                fresh = alpha * xw[index] + beta * xslot[slot, index]
                xw[index] = fresh
                fresh = keep * xg[index] + fresh
                xg[index] = fresh
                for upward in range(-2, 3):
                    xr[index, upward + 2, :, pl.ds(EDGE, cols), :] = rolled(
                        fresh[: 6 * cols], upward).reshape(6, cols, depth)
        for side in range(2):
            face_forces(0, side, -1.0 if side == 0 else 1.0)
        for side in (near_side, 1 - near_side):
            step_y = 2 * side - 1
            there_y = (my_y + step_y >= 0) & (my_y + step_y < ny)
            for step_x in (0, -1, 1):
                if step_x == 0:
                    there, index, here = there_y, 2 + side, pl.ds(16, rows * 8)
                    src = ypack.at[slot, side]
                else:
                    there = there_y & sides[0 if step_x < 0 else 1][2]
                    index = (4 if step_x < 0 else 6) + side
                    here = pl.ds(0 if step_x < 0 else (rows + 2) * 8, 16)
                    src = ypack.at[slot, side, pl.ds(0, 16)]

                @pl.when(there)
                def _():
                    copy = pltpu.make_async_remote_copy(
                        src_ref=src, dst_ref=yslot.at[slot, side, here],
                        send_sem=send_sem.at[slot, index], recv_sem=recv_sem.at[slot, index],
                        device_id=(my_x + step_x, my_y + step_y), device_id_type=MESH,
                    )
                    copy.wait_send()
                    copy.wait_recv()
                    fresh = alpha * yw[side, here] + beta * yslot[slot, side, here]
                    yw[side, here] = fresh
                    yg[side, here] = keep * yg[side, here] + fresh
            for upward in range(-2, 3):
                yr[side, upward + 2] = rolled(yg[side], upward)
            face_forces(1, side, jnp.where(side == 0, -1.0, 1.0))

        @pl.when(turn == 0)
        def _():
            fetches[3].wait()
            fetches[4].wait()
            for c in range(3):
                whole = force[c] + flags[...].astype(f32) * load[c]
                force[c] = whole
                total[c] = whole

        @pl.when(turn < ITERS)
        def _():
            pack(force, lax.rem(turn + 2, SLOTS))

        @pl.when(turn == 0)
        def _():
            for c in range(3):
                set_pad(c, speed[c])

        @pl.when(turn == 1)
        def _():
            for c in range(3):
                change[c] = force[c]
                set_pad(c, total[c])
            acc[0] = dot(speed, speed)
            acc[1] = dot(speed, total)
            acc[2] = dot(total, total)
            acc[3] = dot(speed, force)
            acc[4] = dot(force, total)
            pl.semaphore_wait(ready, ny - 1)
            send_sums(0)

        @pl.when(turn >= 2)
        def _():
            acc[5] = dot(total, force)
            send_sums(lax.rem(turn - 1, SLOTS))
            alpha, beta = take_sums(lax.rem(turn - 2, SLOTS))
            sums = [None] * 5
            for c in range(3):
                w = alpha * change[c] + beta * force[c]
                v = alpha * speed[c] + beta * total[c]
                g = total[c] + w
                change[c] = w
                speed[c] = v
                total[c] = g
                field[c] = field[c] + v
                set_pad(c, g)
                for which, (a, b) in enumerate(((v, v), (v, g), (g, g), (v, w), (w, g))):
                    sums[which] = add(sums[which], jnp.sum((a * b).reshape(-1, 8, depth), axis=0))
            for which in range(5):
                acc[which] = sums[which]

        return carry

    lax.fori_loop(0, ITERS + 1, step, 0)
    alpha, beta = take_sums((ITERS - 1) % SLOTS)
    for c in range(3):
        v = alpha * speed[c] + beta * total[c]
        speed[c] = v
        field[c] = field[c] + v


def on_device(nx, ny, disp, vel, load, flags, mask_bits):
    parts, rows, cols, depth = disp.shape
    words = mask_bits.shape[0]
    cells = rows * cols
    f32, i32 = jnp.float32, jnp.int32
    vmem, dma = pltpu.VMEM, pltpu.SemaphoreType.DMA
    wide = cols + 2 * EDGE
    flat = (parts, cells, depth)
    tall = (rows + 6) * cols
    ring = (rows + 4) * 8
    scratch = [
        vmem(flat, f32),
        vmem((cells, depth), i32),
        vmem((words, cells, depth), i32),
        vmem((len(TABLE), cells, depth), f32),
        vmem((6, cells, depth), f32),
        vmem((parts, rows + 6, wide, depth), f32),
        vmem((words, rows + 6, wide, depth), i32),
        vmem((parts, tall, depth), f32),
        vmem((words, tall, depth), i32),
        vmem((2, tall, depth), f32),
        vmem((2, tall, depth), f32),
        vmem(flat, f32),
        vmem(flat, f32),
        vmem(flat, f32),
        vmem((2, len(FACE), cols, depth), f32),
        vmem((2, len(FACE), rows, depth), f32),
        vmem((2, 7 * cols, depth), f32),
        vmem((2, 7 * cols, depth), f32),
        vmem((2, ring, depth), f32),
        vmem((2, ring, depth), f32),
        vmem((2, 5, 6, wide, depth), f32),
        vmem((2, 5, ring, depth), f32),
        vmem((2, 5, 8, wide, depth), i32),
        vmem((2, 5, ring, depth), i32),
        vmem((2, cols, depth), i32),
        vmem((2, rows, depth), i32),
        vmem((SLOTS, 2, 7 * cols, depth), f32),
        vmem((SLOTS, 2, rows * 8, depth), f32),
        vmem((SLOTS, 2, 7 * cols, depth), f32),
        vmem((SLOTS, 2, ring, depth), f32),
        vmem((2, 9 * cols, depth), i32),
        vmem((2, rows * 8, depth), i32),
        vmem((2, rows, depth), i32),
        vmem((2, 9 * cols, depth), i32),
        vmem((2, ring, depth), i32),
        vmem((2, rows, depth), i32),
        vmem((6, 8, depth), f32),
        vmem((8, depth), f32),
        vmem((SLOTS, 1, depth), f32),
        vmem((SLOTS, nx * ny - 1, 1, depth), f32),
        dma((5,)),
        dma((SLOTS, 8)),
        dma((SLOTS, 8)),
        dma((2, 8)),
        dma((2, 8)),
        dma((SLOTS,)),
        dma((SLOTS,)),
        pltpu.SemaphoreType.REGULAR,
    ]
    outs = pl.pallas_call(
        functools.partial(kernel, nx, ny),
        out_shape=[jax.ShapeDtypeStruct(flat, f32)] * 2,
        in_specs=[pl.BlockSpec(memory_space=pltpu.HBM)] * 5,
        out_specs=[pl.BlockSpec(memory_space=pltpu.VMEM)] * 2,
        scratch_shapes=scratch,
        compiler_params=pltpu.CompilerParams(
            has_side_effects=True, collective_id=0, vmem_limit_bytes=67043328),
    )(disp.reshape(flat), vel.reshape(flat), load.reshape(flat), flags.reshape(cells, depth),
      mask_bits.reshape(words, cells, depth))
    return tuple(out.reshape(disp.shape) for out in outs)


def solution(mesh):
    cells = P(None, "gx", "gy", None)
    return jax.shard_map(
        functools.partial(on_device, mesh.shape["gx"], mesh.shape["gy"]),
        mesh=mesh,
        in_specs=(cells, cells, cells, P("gx", "gy", None), cells),
        out_specs=(cells, cells),
        check_vma=False,
    )
```

```python
import functools
import math

import jax
import jax.numpy as jnp
from jax import lax
from jax.experimental import pallas as pl
from jax.experimental.pallas import tpu as pltpu
from jax.sharding import PartitionSpec as P

ITERS = 8
MESH = pl.DeviceIdType.MESH

fictive_mass = 64.0
epsilon = 1e-06

EDGE = 8
SLOTS = 4
EARLY = 3
DEEP = 7


def neighbour_table():
    table = []
    for across in range(-3, 4):
        for along in range(-3, 4):
            for upward in range(-3, 4):
                length = across * across + along * along + upward * upward
                if 0 < length <= 9:
                    table.append((across, along, upward))
    return table


TABLE = neighbour_table()
NUMBER = {offset: number for number, offset in enumerate(TABLE)}

PLANES = [(1, 0), (1, 1), (2, 0)]
LONG = [(1, 2), (2, 1), (3, 0)]


def reach(along, upward):
    return [a for a in range(-3, 4) if (a, along, upward) in NUMBER]


def crossing(layer, r):
    far = layer + r
    return [(p, c) for c in range(-2, 3) for p in range(-2, 3) if far * far + p * p + c * c <= 9]


SLOT = {(0, 0): 0, (0, 1): 1, (0, 2): 2, (1, 1): 3, (1, 2): 4, (2, 2): 5}
FACE = {}
for plane in PLANES:
    for offset in crossing(*plane):
        FACE[plane + offset] = len(FACE)
for plane in LONG:
    FACE[plane + (0, 0)] = len(FACE)


def bond(offset):
    number = NUMBER[offset]
    word, bit = divmod(number, 31)
    mirror_word, mirror_bit = divmod(121 - number, 31)
    length = float(sum(part * part for part in offset))
    return word, 1 << bit, mirror_word, 1 << mirror_bit, 1.0 / (length * math.sqrt(length))


FACE_WORDS = [
    sorted({bond((sign * (layer + r), p, c))[2] for layer, r, p, c in FACE}) for sign in (-1, 1)
]
KEPT = max(len(words) for words in FACE_WORDS)


def rolled(cells, upward):
    depth = cells.shape[-1]
    if upward == 0:
        return cells
    return pltpu.roll(cells, (-upward) % depth, cells.ndim - 1)


def add(total, term):
    return term if total is None else total + term


def scaled(scale, value):
    return value if scale == 1 else float(scale) * value


def kernel(
    nx, ny,
    disp_in, vel_in, load_in, flags_in, mask_in,
    field, speed,
    load, flags, mask,
    weights, diagonal, pad, mask_pad, shifted, mask_shifted, mixed, plain, force, total, change,
    wx, wy, xg, xw, yg, yw, xr, yr, mxr, myr, mx3, my3,
    xpack, ypack, xslot, yslot, mxpack, mypack, my3pack, mxslot, myslot, my3slot,
    acc, ab, sums_out, sums_in,
    local_sem, send_sem, recv_sem, msend_sem, mrecv_sem, sum_send_sem, sum_recv_sem, ready,
):
    depth = flags.shape[-1]
    cells = flags.shape[0]
    rows = pad.shape[1] - 6
    cols = cells // rows
    count = 3.0 * rows * nx * cols * ny * depth
    my_x = lax.axis_index("gx")
    my_y = lax.axis_index("gy")
    f32, i32 = jnp.float32, jnp.int32

    fetches = [
        pltpu.make_async_copy(src, dst, local_sem.at[index])
        for index, (src, dst) in enumerate((
            (mask_in, mask), (disp_in, field), (vel_in, speed), (load_in, load), (flags_in, flags),
        ))
    ]
    for fetch in fetches:
        fetch.start()

    sides = []
    for step_x, step_y in ((-1, 0), (1, 0), (0, -1), (0, 1), (-1, -1), (-1, 1), (1, -1), (1, 1)):
        there = None
        for step, mine, size in ((step_x, my_x, nx), (step_y, my_y, ny)):
            if step:
                near = mine > 0 if step < 0 else mine < size - 1
                there = near if there is None else there & near
        sides.append((step_x, step_y, there))

    barrier = pltpu.get_barrier_semaphore()
    peers = nx + ny - 2
    for step_x, step_y, there in sides[4:]:
        @pl.when(there)
        def _():
            pl.semaphore_signal(barrier, inc=1, device_id=(my_x + step_x, my_y + step_y), device_id_type=MESH)
        peers = peers + there.astype(i32)
    for hop in range(1, ny):
        pl.semaphore_signal(barrier, inc=1, device_id=(my_x, lax.rem(my_y + hop, ny)), device_id_type=MESH)
    for hop in range(1, nx):
        pl.semaphore_signal(barrier, inc=1, device_id=(lax.rem(my_x + hop, nx), my_y), device_id_type=MESH)

    def opposite(index):
        return index ^ 1 if index < 4 else 11 - index

    def outgoing(index, slot):
        step_x, step_y, _ = sides[index]
        if index < 2:
            src, dst = xpack.at[slot, index], xslot.at[slot, 1 - index]
        elif index < 4:
            src, dst = ypack.at[slot, index - 2], yslot.at[slot, 3 - index, pl.ds(2 * DEEP, rows * DEEP)]
        else:
            side = 0 if step_y < 0 else 1
            start = 0 if step_x < 0 else rows - 2
            land = rows + 2 if step_x < 0 else 0
            src = ypack.at[slot, side, pl.ds(start * DEEP, 2 * DEEP - 1)]
            dst = yslot.at[slot, 1 - side, pl.ds(land * DEEP, 2 * DEEP - 1)]
        return pltpu.make_async_remote_copy(
            src_ref=src, dst_ref=dst, send_sem=send_sem.at[slot, index], recv_sem=recv_sem.at[slot, opposite(index)],
            device_id=(my_x + step_x, my_y + step_y), device_id_type=MESH,
        )

    def outgoing_mask(index):
        step_x, step_y, _ = sides[index]
        if index < 2:
            pairs = [(mxpack.at[index], mxslot.at[1 - index])]
        elif index < 4:
            pairs = [
                (mypack.at[index - 2], myslot.at[3 - index, pl.ds(2 * 8, rows * 8)]),
                (my3pack.at[index - 2], my3slot.at[3 - index]),
            ]
        else:
            side = 0 if step_y < 0 else 1
            start = 0 if step_x < 0 else rows - 2
            land = rows + 2 if step_x < 0 else 0
            pairs = [(mypack.at[side, pl.ds(start * 8, 16)], myslot.at[1 - side, pl.ds(land * 8, 16)])]
        return [
            pltpu.make_async_remote_copy(
                src_ref=src, dst_ref=dst, send_sem=msend_sem.at[part, index],
                recv_sem=mrecv_sem.at[part, opposite(index)],
                device_id=(my_x + step_x, my_y + step_y), device_id_type=MESH,
            )
            for part, (src, dst) in enumerate(pairs)
        ]

    ORDER = (4, 5, 6, 7, 2, 3, 0, 1)

    def column(at):
        return pl.ds(at, rows, stride=cols)

    def spread(at, deep=DEEP):
        return pl.ds(at, rows, stride=deep)

    def send_y(source, slot, side):
        step_y = 2 * side - 1
        there_y = (my_y + step_y >= 0) & (my_y + step_y < ny)
        for layer in (1, 2, 3):
            at = jnp.where(side == 0, layer - 1, cols - layer)
            for c in range(3) if layer < 3 else (1,):
                e = 3 * (layer - 1) + (c if layer < 3 else 0)
                ypack[slot, side, spread(e), :] = source[c, column(at), :]
        for step_x in (-1, 1, 0):
            if step_x == 0:
                there, index, other = there_y, 2 + side, 3 - side
                src, dst = ypack.at[slot, side], yslot.at[slot, 1 - side, pl.ds(2 * DEEP, rows * DEEP)]
            else:
                there = there_y & sides[0 if step_x < 0 else 1][2]
                index = (4 if step_x < 0 else 6) + side
                other = 11 - index
                start = 0 if step_x < 0 else rows - 2
                land = rows + 2 if step_x < 0 else 0
                src = ypack.at[slot, side, pl.ds(start * DEEP, 2 * DEEP - 1)]
                dst = yslot.at[slot, 1 - side, pl.ds(land * DEEP, 2 * DEEP - 1)]

            @pl.when(there)
            def _():
                pltpu.make_async_remote_copy(
                    src_ref=src, dst_ref=dst, send_sem=send_sem.at[slot, index], recv_sem=recv_sem.at[slot, other],
                    device_id=(my_x + step_x, my_y + step_y), device_id_type=MESH,
                ).start()

    def send_x(source, slot):
        for side in range(2):
            for layer in (1, 2, 3):
                at = layer - 1 if side == 0 else rows - layer
                for c in range(3) if layer < 3 else (0,):
                    e = 3 * (layer - 1) + c
                    xpack[slot, side, pl.ds(e * cols, cols), :] = source[c, pl.ds(at * cols, cols), :]
        for index in (0, 1):
            @pl.when(sides[index][2])
            def _():
                outgoing(index, slot).start()

    near_side = 1 - lax.rem(my_y, 2)

    def pack(source, slot):
        send_y(source, slot, 1 - near_side)
        send_y(source, slot, near_side)
        send_x(source, slot)

    def arrived(index, slot):
        outgoing(index, slot).wait_send()
        outgoing(opposite(index), slot).wait_recv()

    pad[...] = jnp.zeros_like(pad)
    mask_pad[...] = jnp.full_like(mask_pad, -1)
    diagonal[...] = jnp.zeros_like(diagonal)
    for state in (xg, xw, yg, yw, xr, ypack, acc):
        state[...] = jnp.zeros_like(state)
    for state in (mxr, myr, mx3, my3, mypack):
        state[...] = jnp.full_like(state, -1)
    ab[...] = jnp.where(lax.broadcasted_iota(i32, ab.shape, 0) == 0, 1.0, 0.0).astype(f32)
    place = lax.broadcasted_iota(i32, (1, depth), 1)
    fetches[0].wait()
    for word in range(4):
        for r in range(rows):
            mask_pad[word, 3 + r, pl.ds(EDGE, cols), :] = mask[word, pl.ds(r * cols, cols), :]

    for side in range(2):
        for layer in (1, 2):
            at = layer - 1 if side == 0 else cols - layer
            for word in range(4):
                mypack[side, spread(4 * (layer - 1) + word, 8), :] = mask[word, column(at), :]
            at = layer - 1 if side == 0 else rows - layer
            for kept, word in enumerate(FACE_WORDS[1 - side]):
                e = KEPT * (layer - 1) + kept
                mxpack[side, pl.ds(e * cols, cols), :] = mask[word, pl.ds(at * cols, cols), :]
        sign = 1 if side == 0 else -1
        word = bond((0, 3 * sign, 0))[2]
        my3pack[side] = mask[word, column(2 if side == 0 else cols - 3), :]
        word = bond((3 * sign, 0, 0))[2]
        mxpack[side, pl.ds(2 * KEPT * cols, cols), :] = mask[word, pl.ds((2 if side == 0 else rows - 3) * cols, cols), :]

    def own_weights(along):
        for word in range(4):
            mask_shifted[word] = mask_pad[word, :, pl.ds(EDGE + along, cols), :].reshape(-1, depth)
        for upward in range(-3, 4):
            across_all = reach(along, upward)
            if not across_all:
                continue
            inside = (place + upward >= 0) & (place + upward < depth)
            for low in range(0, rows, 4):
                here = pl.ds(low * cols, 4 * cols)
                moments = [None, None, None]
                for across in across_all:
                    word, bit, mirror_word, mirror_bit, weight = bond((across, along, upward))
                    own = mask[word, here] & bit
                    far = mask_shifted[mirror_word, pl.ds((3 + low + across) * cols, 4 * cols)] & mirror_bit
                    far = rolled(jnp.where(far == 0, f32(weight), f32(0.0)), upward)
                    one = jnp.where((own == 0) & inside, far, f32(0.0))
                    weights[NUMBER[(across, along, upward)], here] = one
                    for power in range(3):
                        scale = across**power
                        if scale:
                            moments[power] = add(moments[power], scaled(scale, one))
                for slot, (power, scale) in enumerate((
                    (2, 1), (1, along), (1, upward), (0, along * along), (0, along * upward), (0, upward * upward),
                )):
                    if scale and moments[power] is not None:
                        diagonal[slot, here] += scaled(scale, moments[power])

    for along in range(-3, -3 + EARLY):
        own_weights(along)
    pl.semaphore_wait(barrier, peers)
    for hop in range(1, ny):
        pl.semaphore_signal(ready, inc=1, device_id=(my_x, lax.rem(my_y + hop, ny)), device_id_type=MESH)
    for index in ORDER:
        @pl.when(sides[index][2])
        def _():
            for copy in outgoing_mask(index):
                copy.start()
    fetches[1].wait()
    pack(field, 0)
    fetches[2].wait()
    pack(speed, 1)
    for along in range(-3 + EARLY, 4):
        own_weights(along)

    middle = (slice(None), pl.ds(3, rows), pl.ds(EDGE, cols), slice(None))

    def set_pad(c, value):
        pad[c, pl.ds(3, rows), pl.ds(EDGE, cols), :] = value.reshape(rows, cols, depth)

    def face_weights(axis, side):
        sign = -1 if side == 0 else 1
        terms, powers = {}, {}
        for layer, r in PLANES + LONG:
            for p, c in crossing(layer, r) if (layer, r) in PLANES else [(0, 0)]:
                out = sign * (layer + r)
                offset = (out, p, c) if axis == 0 else (p, out, c)
                word, bit, mirror_word, mirror_bit, weight = bond(offset)
                if axis == 0:
                    at = r if side == 0 else rows - 1 - r
                    own = mask[word, pl.ds(at * cols, cols), :]
                    if layer == 3:
                        far = mx3[side]
                    else:
                        kept = KEPT * (layer - 1) + FACE_WORDS[side].index(mirror_word)
                        far = mxr[side, c + 2, kept, pl.ds(EDGE + p, cols), :]
                else:
                    at = r if side == 0 else cols - 1 - r
                    own = mask[word, column(at), :]
                    if layer == 3:
                        far = my3[side]
                    else:
                        far = myr[side, c + 2, spread((2 + p) * 8 + 4 * (layer - 1) + mirror_word, 8), :]
                one = jnp.where(((own & bit) | (far & mirror_bit)) == 0, f32(weight), f32(0.0))
                if axis == 0:
                    wx[side, FACE[layer, r, p, c]] = one
                else:
                    wy[side, FACE[layer, r, p, c]] = one
                for power in range(3):
                    if p**power:
                        key = (out, r, c, power)
                        powers[key] = add(powers.get(key), scaled(p**power, one))
        for (out, r, c, power), term in powers.items():
            for parts in ((0, 0), (0, 1), (0, 2), (1, 1), (1, 2), (2, 2)):
                tangent = 1 - axis
                if parts.count(tangent) != power:
                    continue
                scale = out ** parts.count(axis) * c ** parts.count(2)
                if scale:
                    key = (r, SLOT[parts])
                    terms[key] = add(terms.get(key), scaled(scale, term))
        for (r, slot), term in terms.items():
            if axis == 0:
                at = r if side == 0 else rows - 1 - r
                diagonal[slot, pl.ds(at * cols, cols), :] += term
            else:
                at = r if side == 0 else cols - 1 - r
                diagonal[slot, column(at), :] += term

    def take_masks(axis):
        for index in range(2) if axis == 0 else range(2, 8):
            step_x, step_y, there = sides[index]

            @pl.when(there)
            def _():
                for copy in outgoing_mask(index):
                    copy.wait_send()
                for copy in outgoing_mask(opposite(index)):
                    copy.wait_recv()
                for upward in range(-2, 3):
                    inside = (place + upward >= 0) & (place + upward < depth)
                    if index < 2:
                        words = mxslot[index, pl.ds(0, 2 * KEPT * cols), :]
                    elif index < 4:
                        first, size = 2 * 8, rows * 8
                        words = myslot[index - 2, pl.ds(first, size), :]
                    else:
                        first, size = (0 if step_x < 0 else (rows + 2) * 8), 16
                        words = myslot[0 if step_y < 0 else 1, pl.ds(first, size), :]
                    if upward:
                        words = jnp.where(inside, rolled(words, upward), -1)
                    if index < 2:
                        mxr[index, upward + 2, :, pl.ds(EDGE, cols), :] = words.reshape(2 * KEPT, cols, depth)
                    else:
                        myr[0 if step_y < 0 else 1, upward + 2, pl.ds(first, size), :] = words
                if index < 2:
                    mx3[index] = mxslot[index, pl.ds(2 * KEPT * cols, cols), :]
                elif index < 4:
                    my3[index - 2] = my3slot[index - 2]
        for side in range(2):
            face_weights(axis, side)

    def own_forces():
        turn = 0
        for low in range(0, rows, 4):
            for c in range(3):
                force[c, pl.ds(low * cols, 4 * cols)] = jnp.zeros((4 * cols, depth), f32)
        for along in range(-3, 4):
            for c in range(3):
                shifted[c] = pad[c, :, pl.ds(EDGE + along, cols), :].reshape(-1, depth)
            for upward in range(-3, 4):
                across_all = reach(along, upward)
                if not across_all:
                    continue
                turn = 1 - turn
                most = max(across_all)
                span = pl.ds(3 * cols, rows * cols)
                if along or upward:
                    mix = None
                    for scale, c in ((along, 1), (upward, 2)):
                        if scale:
                            mix = add(mix, scaled(scale, shifted[c, span]))
                    mixed[turn, span] = rolled(mix, upward)
                if most:
                    plain[turn, span] = rolled(shifted[0, span], upward)
                for low in range(0, rows, 4):
                    here = pl.ds(low * cols, 4 * cols)
                    whole = None
                    lean = None

                    def stretch(across):
                        at = pl.ds((3 + low + across) * cols, 4 * cols)
                        value = mixed[turn, at] if along or upward else None
                        if across:
                            term = float(across) * plain[turn, at]
                            value = term if value is None else value + term
                        return weights[NUMBER[(across, along, upward)], here] * value

                    for across in [a for a in across_all if a >= 0]:
                        if across == 0:
                            whole = stretch(0)
                            continue
                        up, down = stretch(across), stretch(-across)
                        both = up + down
                        whole = both if whole is None else whole + both
                        lean = add(lean, scaled(across, up - down))
                    if lean is not None:
                        force[0, here] += lean
                    if along:
                        force[1, here] += float(along) * whole
                    if upward:
                        force[2, here] += float(upward) * whole

    def diagonal_forces():
        for low in range(0, rows, 4):
            here = pl.ds(low * cols, 4 * cols)
            u = [pad[c, pl.ds(3 + low, 4), pl.ds(EDGE, cols), :].reshape(4 * cols, depth) for c in range(3)]
            d = [diagonal[slot, here] for slot in range(6)]
            force[0, here] -= d[0] * u[0] + d[1] * u[1] + d[2] * u[2]
            force[1, here] -= d[1] * u[0] + d[3] * u[1] + d[4] * u[2]
            force[2, here] -= d[2] * u[0] + d[4] * u[1] + d[5] * u[2]

    def face_forces(axis, side, sign):
        normal, tangent = (0, 1) if axis == 0 else (1, 0)
        result = {}
        for layer in (1, 2):
            inner = [r for one, r in PLANES if one == layer]
            wide = {}
            for c in range(-2, 3):
                sums = {}
                for p in range(-2, 3):
                    targets = [r for r in inner if (layer, r, p, c) in FACE]
                    if not targets:
                        continue

                    def near(component):
                        e = 3 * (layer - 1) + component
                        if axis == 0:
                            return xr[side, c + 2, e, pl.ds(EDGE + p, cols), :]
                        return yr[side, c + 2, spread((2 + p) * DEEP + e), :]

                    out = sign * near(normal)
                    base = None
                    if p:
                        base = scaled(p, near(tangent))
                    if c:
                        base = add(base, scaled(c, near(2)))
                    for r in targets:
                        value = scaled(layer + r, out)
                        if base is not None:
                            value = value + base
                        one = (wx if axis == 0 else wy)[side, FACE[layer, r, p, c]] * value
                        sums[r, 0] = add(sums.get((r, 0)), one)
                        if p:
                            sums[r, 1] = add(sums.get((r, 1)), scaled(p, one))
                for r in inner:
                    if (r, 0) not in sums:
                        continue
                    wide[r, normal] = add(wide.get((r, normal)), sums[r, 0])
                    if (r, 1) in sums:
                        wide[r, tangent] = add(wide.get((r, tangent)), sums[r, 1])
                    if c:
                        wide[r, 2] = add(wide.get((r, 2)), scaled(c, sums[r, 0]))
            for r in inner:
                wide[r, normal] = sign * scaled(layer + r, wide[r, normal])
                for component in range(3):
                    result[r, component] = add(result.get((r, component)), wide[r, component])
        for layer, r in LONG:
            e = 6 if layer == 3 else 3 * (layer - 1) + normal
            if axis == 0:
                out = xg[side, pl.ds(e * cols, cols), :]
            else:
                out = yg[side, spread(2 * DEEP + e), :]
            one = 9.0 * ((wx if axis == 0 else wy)[side, FACE[layer, r, 0, 0]] * out)
            result[r, normal] = add(result.get((r, normal)), one)
        for (r, component), term in result.items():
            if axis == 0:
                at = r if side == 0 else rows - 1 - r
                force[component, pl.ds(at * cols, cols), :] += term
            else:
                at = jnp.where(side == 0, r, cols - 1 - r)
                force[component, column(at), :] += term

    hops = [(hop_x, hop_y) for hop_y in range(ny) for hop_x in range(nx) if hop_x or hop_y]
    hops.sort(key=lambda hop: (abs(2 * hop[1] - ny), abs(2 * hop[0] - nx)))

    def dot(first, second):
        whole = None
        for c in range(3):
            whole = add(whole, jnp.sum((first[c] * second[c]).reshape(-1, 8, depth), axis=0))
        return whole

    def send_sums(slot):
        line = jnp.zeros((1, depth), f32)
        for which in range(6):
            one = jnp.sum(jnp.sum(acc[which], axis=0, keepdims=True), axis=1, keepdims=True)
            line = jnp.where(place == which, one, line)
        sums_out[slot] = line

        for which, (hop_x, hop_y) in enumerate(hops):
            pltpu.make_async_remote_copy(
                src_ref=sums_out.at[slot], dst_ref=sums_in.at[slot, which],
                send_sem=sum_send_sem.at[slot], recv_sem=sum_recv_sem.at[slot],
                device_id=(lax.rem(my_x + hop_x, nx), lax.rem(my_y + hop_y, ny)), device_id_type=MESH,
            ).start()

    def take_sums(slot):
        whole = sums_in.at[slot]
        pltpu.make_async_copy(whole, whole, sum_send_sem.at[slot]).wait()
        pltpu.make_async_copy(whole, whole, sum_recv_sem.at[slot]).wait()
        line = jnp.sum(sums_in[slot], axis=0) + sums_out[slot]
        vv, vg, gg, vw, wg, gh = [
            jnp.sum(jnp.where(place == which, line, 0.0), axis=1, keepdims=True) for which in range(6)
        ]
        alpha, beta = ab[0:1, 0:1], ab[1:2, 0:1]
        kinetic = alpha * alpha * vv + 2.0 * alpha * beta * vg + beta * beta * gg
        rayleigh = -(alpha * alpha * vw + 2.0 * alpha * beta * wg + beta * beta * gh)
        damping = 2.0 * jnp.sqrt(rayleigh / count / (fictive_mass * (kinetic / count + epsilon)))
        alpha = (2.0 - damping) / (2.0 + damping)
        beta = 2.0 / (fictive_mass * (2.0 + damping))
        ab[0:1, :] = jnp.broadcast_to(alpha, (1, depth))
        ab[1:2, :] = jnp.broadcast_to(beta, (1, depth))
        return alpha, beta

    def step(turn, carry):
        @pl.when(turn != 1)
        def _():
            own_forces()

        @pl.when(turn == 0)
        def _():
            take_masks(0)

        @pl.when(turn == 1)
        def _():
            for c in range(3):
                force[c] = change[c]

        sent = lax.rem(turn + 2, SLOTS)
        slot = jnp.where(turn < 3, turn, lax.rem(turn + 1, SLOTS))
        early = turn < 3
        alpha = jnp.where(early, 0.0, ab[0:1, :])
        beta = jnp.where(early, 1.0, ab[1:2, :])
        keep = jnp.where(early, 0.0, jnp.ones((1, depth), f32))

        @pl.when(turn == 3)
        def _():
            for index in range(8):
                step_x, step_y, there = sides[index]

                @pl.when(there)
                def _():
                    arrived(index, 3)
                    if index < 2:
                        xw[index] = xslot[3, index]
                    else:
                        side = 0 if step_y < 0 else 1
                        here = pl.ds(2 * DEEP, rows * DEEP) if index < 4 else pl.ds(0 if step_x < 0 else (rows + 2) * DEEP, 2 * DEEP - 1)
                        yw[side, here] = yslot[3, side, here]

        for index in (0, 1):
            @pl.when(sides[index][2])
            def _():
                arrived(index, slot)
                fresh = alpha * xw[index] + beta * xslot[slot, index]
                xw[index] = fresh
                fresh = keep * xg[index] + fresh
                xg[index] = fresh
                for upward in range(-2, 3):
                    xr[index, upward + 2, :, pl.ds(EDGE, cols), :] = rolled(
                        fresh[: 6 * cols], upward).reshape(6, cols, depth)
        for side in range(2):
            face_forces(0, side, -1.0 if side == 0 else 1.0)

        @pl.when(turn == 0)
        def _():
            take_masks(1)

        diagonal_forces()

        @pl.when(turn == 0)
        def _():
            fetches[3].wait()
            fetches[4].wait()
            for c in range(3):
                force[c] += flags[...].astype(f32) * load[c]

        for side in (near_side, 1 - near_side):
            step_y = 2 * side - 1
            there_y = (my_y + step_y >= 0) & (my_y + step_y < ny)
            for step_x in (0, -1, 1):
                if step_x == 0:
                    there, index, here = there_y, 2 + side, pl.ds(2 * DEEP, rows * DEEP)
                    src = ypack.at[slot, side]
                else:
                    there = there_y & sides[0 if step_x < 0 else 1][2]
                    index = (4 if step_x < 0 else 6) + side
                    here = pl.ds(0 if step_x < 0 else (rows + 2) * DEEP, 2 * DEEP - 1)
                    src = ypack.at[slot, side, pl.ds(0, 2 * DEEP - 1)]

                @pl.when(there)
                def _():
                    copy = pltpu.make_async_remote_copy(
                        src_ref=src, dst_ref=yslot.at[slot, side, here],
                        send_sem=send_sem.at[slot, index], recv_sem=recv_sem.at[slot, index],
                        device_id=(my_x + step_x, my_y + step_y), device_id_type=MESH,
                    )
                    copy.wait_send()
                    copy.wait_recv()
                    fresh = alpha * yw[side, here] + beta * yslot[slot, side, here]
                    yw[side, here] = fresh
                    yg[side, here] = keep * yg[side, here] + fresh
            for upward in range(-2, 3):
                yr[side, upward + 2] = rolled(yg[side], upward)
            face_forces(1, side, jnp.where(side == 0, -1.0, 1.0))

            @pl.when(turn < ITERS)
            def _():
                send_y(force, sent, side)

        @pl.when(turn < ITERS)
        def _():
            send_x(force, sent)

        @pl.when(turn == 0)
        def _():
            for c in range(3):
                total[c] = force[c]
                set_pad(c, speed[c])

        @pl.when(turn == 1)
        def _():
            for c in range(3):
                change[c] = force[c]
                set_pad(c, total[c])
            acc[0] = dot(speed, speed)
            acc[1] = dot(speed, total)
            acc[2] = dot(total, total)
            acc[3] = dot(speed, force)
            acc[4] = dot(force, total)
            pl.semaphore_wait(ready, ny - 1)
            send_sums(0)

        @pl.when(turn >= 2)
        def _():
            acc[5] = dot(total, force)
            send_sums(lax.rem(turn - 1, SLOTS))
            alpha, beta = take_sums(lax.rem(turn - 2, SLOTS))
            sums = [None] * 5
            for c in range(3):
                w = alpha * change[c] + beta * force[c]
                v = alpha * speed[c] + beta * total[c]
                g = total[c] + w
                change[c] = w
                speed[c] = v
                total[c] = g
                field[c] = field[c] + v
                set_pad(c, g)
                for which, (a, b) in enumerate(((v, v), (v, g), (g, g), (v, w), (w, g))):
                    sums[which] = add(sums[which], jnp.sum((a * b).reshape(-1, 8, depth), axis=0))
            for which in range(5):
                acc[which] = sums[which]

        return carry

    for c in range(3):
        set_pad(c, speed[c])
    own_forces()
    for c in range(3):
        change[c] = force[c]
        set_pad(c, field[c])
    lax.fori_loop(0, ITERS + 1, step, 0)
    alpha, beta = take_sums((ITERS - 1) % SLOTS)
    for c in range(3):
        v = alpha * speed[c] + beta * total[c]
        speed[c] = v
        field[c] = field[c] + v


def on_device(nx, ny, disp, vel, load, flags, mask_bits):
    parts, rows, cols, depth = disp.shape
    words = mask_bits.shape[0]
    cells = rows * cols
    f32, i32 = jnp.float32, jnp.int32
    vmem, dma = pltpu.VMEM, pltpu.SemaphoreType.DMA
    wide = cols + 2 * EDGE
    flat = (parts, cells, depth)
    tall = (rows + 6) * cols
    ring = (rows + 4) * 8
    deep = (rows + 4) * DEEP
    scratch = [
        vmem(flat, f32),
        vmem((cells, depth), i32),
        vmem((words, cells, depth), i32),
        vmem((len(TABLE), cells, depth), f32),
        vmem((6, cells, depth), f32),
        vmem((parts, rows + 6, wide, depth), f32),
        vmem((words, rows + 6, wide, depth), i32),
        vmem((parts, tall, depth), f32),
        vmem((words, tall, depth), i32),
        vmem((2, tall, depth), f32),
        vmem((2, tall, depth), f32),
        vmem(flat, f32),
        vmem(flat, f32),
        vmem(flat, f32),
        vmem((2, len(FACE), cols, depth), f32),
        vmem((2, len(FACE), rows, depth), f32),
        vmem((2, 7 * cols, depth), f32),
        vmem((2, 7 * cols, depth), f32),
        vmem((2, deep, depth), f32),
        vmem((2, deep, depth), f32),
        vmem((2, 5, 6, wide, depth), f32),
        vmem((2, 5, deep, depth), f32),
        vmem((2, 5, 2 * KEPT, wide, depth), i32),
        vmem((2, 5, ring, depth), i32),
        vmem((2, cols, depth), i32),
        vmem((2, rows, depth), i32),
        vmem((SLOTS, 2, 7 * cols, depth), f32),
        vmem((SLOTS, 2, rows * DEEP, depth), f32),
        vmem((SLOTS, 2, 7 * cols, depth), f32),
        vmem((SLOTS, 2, deep, depth), f32),
        vmem((2, (2 * KEPT + 1) * cols, depth), i32),
        vmem((2, rows * 8, depth), i32),
        vmem((2, rows, depth), i32),
        vmem((2, (2 * KEPT + 1) * cols, depth), i32),
        vmem((2, ring, depth), i32),
        vmem((2, rows, depth), i32),
        vmem((6, 8, depth), f32),
        vmem((8, depth), f32),
        vmem((SLOTS, 1, depth), f32),
        vmem((SLOTS, nx * ny - 1, 1, depth), f32),
        dma((5,)),
        dma((SLOTS, 8)),
        dma((SLOTS, 8)),
        dma((2, 8)),
        dma((2, 8)),
        dma((SLOTS,)),
        dma((SLOTS,)),
        pltpu.SemaphoreType.REGULAR,
    ]
    outs = pl.pallas_call(
        functools.partial(kernel, nx, ny),
        out_shape=[jax.ShapeDtypeStruct(flat, f32)] * 2,
        in_specs=[pl.BlockSpec(memory_space=pltpu.HBM)] * 5,
        out_specs=[pl.BlockSpec(memory_space=pltpu.VMEM)] * 2,
        scratch_shapes=scratch,
        compiler_params=pltpu.CompilerParams(
            has_side_effects=True, collective_id=0, vmem_limit_bytes=67043328),
    )(disp.reshape(flat), vel.reshape(flat), load.reshape(flat), flags.reshape(cells, depth),
      mask_bits.reshape(words, cells, depth))
    return tuple(out.reshape(disp.shape) for out in outs)


def solution(mesh):
    cells = P(None, "gx", "gy", None)
    return jax.shard_map(
        functools.partial(on_device, mesh.shape["gx"], mesh.shape["gy"]),
        mesh=mesh,
        in_specs=(cells, cells, cells, P("gx", "gy", None), cells),
        out_specs=(cells, cells),
        check_vma=False,
    )
```

```python
import functools
import math

import jax
import jax.numpy as jnp
from jax import lax
from jax.experimental import pallas as pl
from jax.experimental.pallas import tpu as pltpu
from jax.sharding import PartitionSpec as P

ITERS = 8
MESH = pl.DeviceIdType.MESH

fictive_mass = 64.0
epsilon = 1e-06

EDGE = 8
SLOTS = 4
EARLY = 4
DEEP = 7


def neighbour_table():
    table = []
    for across in range(-3, 4):
        for along in range(-3, 4):
            for upward in range(-3, 4):
                length = across * across + along * along + upward * upward
                if 0 < length <= 9:
                    table.append((across, along, upward))
    return table


TABLE = neighbour_table()
NUMBER = {offset: number for number, offset in enumerate(TABLE)}

PLANES = [(1, 0), (1, 1), (2, 0)]
LONG = [(1, 2), (2, 1), (3, 0)]


def reach(along, upward):
    return [a for a in range(-3, 4) if (a, along, upward) in NUMBER]


def crossing(layer, r):
    far = layer + r
    return [(p, c) for c in range(-2, 3) for p in range(-2, 3) if far * far + p * p + c * c <= 9]


SLOT = {(0, 0): 0, (0, 1): 1, (0, 2): 2, (1, 1): 3, (1, 2): 4, (2, 2): 5}
FACE = {}
for plane in PLANES:
    for offset in crossing(*plane):
        FACE[plane + offset] = len(FACE)
for plane in LONG:
    FACE[plane + (0, 0)] = len(FACE)


def bond(offset):
    number = NUMBER[offset]
    word, bit = divmod(number, 31)
    mirror_word, mirror_bit = divmod(121 - number, 31)
    length = float(sum(part * part for part in offset))
    return word, 1 << bit, mirror_word, 1 << mirror_bit, 1.0 / (length * math.sqrt(length))


FACE_WORDS = [
    sorted({bond((sign * (layer + r), p, c))[2] for layer, r, p, c in FACE}) for sign in (-1, 1)
]
KEPT = max(len(words) for words in FACE_WORDS)


def rolled(cells, upward):
    depth = cells.shape[-1]
    if upward == 0:
        return cells
    return pltpu.roll(cells, (-upward) % depth, cells.ndim - 1)


def add(total, term):
    return term if total is None else total + term


def scaled(scale, value):
    return value if scale == 1 else float(scale) * value


def kernel(
    nx, ny,
    disp_in, vel_in, load_in, flags_in, mask_in,
    field, speed,
    load, flags, mask,
    weights, diagonal, pad, mask_pad, shifted, mask_shifted, mixed, plain, force, total, change,
    wx, wy, xg, xw, yg, yw, xr, yr, mxr, myr, mx3, my3,
    xpack, ypack, xslot, yslot, mxpack, mypack, my3pack, mxslot, myslot, my3slot,
    acc, ab, sums_out, sums_in,
    local_sem, send_sem, recv_sem, msend_sem, mrecv_sem, sum_send_sem, sum_recv_sem, ready,
):
    depth = flags.shape[-1]
    cells = flags.shape[0]
    rows = pad.shape[1] - 6
    cols = cells // rows
    count = 3.0 * rows * nx * cols * ny * depth
    my_x = lax.axis_index("gx")
    my_y = lax.axis_index("gy")
    f32, i32 = jnp.float32, jnp.int32

    fetches = [
        pltpu.make_async_copy(src, dst, local_sem.at[index])
        for index, (src, dst) in enumerate((
            (mask_in, mask), (disp_in, field), (vel_in, speed), (load_in, load), (flags_in, flags),
        ))
    ]
    for fetch in fetches:
        fetch.start()

    sides = []
    for step_x, step_y in ((-1, 0), (1, 0), (0, -1), (0, 1), (-1, -1), (-1, 1), (1, -1), (1, 1)):
        there = None
        for step, mine, size in ((step_x, my_x, nx), (step_y, my_y, ny)):
            if step:
                near = mine > 0 if step < 0 else mine < size - 1
                there = near if there is None else there & near
        sides.append((step_x, step_y, there))

    barrier = pltpu.get_barrier_semaphore()
    peers = nx + ny - 2
    for step_x, step_y, there in sides[4:]:
        @pl.when(there)
        def _():
            pl.semaphore_signal(barrier, inc=1, device_id=(my_x + step_x, my_y + step_y), device_id_type=MESH)
        peers = peers + there.astype(i32)
    for hop in range(1, ny):
        pl.semaphore_signal(barrier, inc=1, device_id=(my_x, lax.rem(my_y + hop, ny)), device_id_type=MESH)
    for hop in range(1, nx):
        pl.semaphore_signal(barrier, inc=1, device_id=(lax.rem(my_x + hop, nx), my_y), device_id_type=MESH)

    def opposite(index):
        return index ^ 1 if index < 4 else 11 - index

    def outgoing(index, slot):
        step_x, step_y, _ = sides[index]
        if index < 2:
            src, dst = xpack.at[slot, index], xslot.at[slot, 1 - index]
        elif index < 4:
            src, dst = ypack.at[slot, index - 2], yslot.at[slot, 3 - index, pl.ds(2 * DEEP, rows * DEEP)]
        else:
            side = 0 if step_y < 0 else 1
            start = 0 if step_x < 0 else rows - 2
            land = rows + 2 if step_x < 0 else 0
            src = ypack.at[slot, side, pl.ds(start * DEEP, 2 * DEEP - 1)]
            dst = yslot.at[slot, 1 - side, pl.ds(land * DEEP, 2 * DEEP - 1)]
        return pltpu.make_async_remote_copy(
            src_ref=src, dst_ref=dst, send_sem=send_sem.at[slot, index], recv_sem=recv_sem.at[slot, opposite(index)],
            device_id=(my_x + step_x, my_y + step_y), device_id_type=MESH,
        )

    def outgoing_mask(index):
        step_x, step_y, _ = sides[index]
        if index < 2:
            pairs = [(mxpack.at[index], mxslot.at[1 - index])]
        elif index < 4:
            pairs = [
                (mypack.at[index - 2], myslot.at[3 - index, pl.ds(2 * 8, rows * 8)]),
                (my3pack.at[index - 2], my3slot.at[3 - index]),
            ]
        else:
            side = 0 if step_y < 0 else 1
            start = 0 if step_x < 0 else rows - 2
            land = rows + 2 if step_x < 0 else 0
            pairs = [(mypack.at[side, pl.ds(start * 8, 16)], myslot.at[1 - side, pl.ds(land * 8, 16)])]
        return [
            pltpu.make_async_remote_copy(
                src_ref=src, dst_ref=dst, send_sem=msend_sem.at[part, index],
                recv_sem=mrecv_sem.at[part, opposite(index)],
                device_id=(my_x + step_x, my_y + step_y), device_id_type=MESH,
            )
            for part, (src, dst) in enumerate(pairs)
        ]

    ORDER = (4, 5, 6, 7, 2, 3, 0, 1)

    def column(at):
        return pl.ds(at, rows, stride=cols)

    def spread(at, deep=DEEP):
        return pl.ds(at, rows, stride=deep)

    def send_y(source, slot, side):
        step_y = 2 * side - 1
        there_y = (my_y + step_y >= 0) & (my_y + step_y < ny)
        for layer in (1, 2, 3):
            at = jnp.where(side == 0, layer - 1, cols - layer)
            for c in range(3) if layer < 3 else (1,):
                e = 3 * (layer - 1) + (c if layer < 3 else 0)
                ypack[slot, side, spread(e), :] = source[c, column(at), :]
        for step_x in (-1, 1, 0):
            if step_x == 0:
                there, index, other = there_y, 2 + side, 3 - side
                src, dst = ypack.at[slot, side], yslot.at[slot, 1 - side, pl.ds(2 * DEEP, rows * DEEP)]
            else:
                there = there_y & sides[0 if step_x < 0 else 1][2]
                index = (4 if step_x < 0 else 6) + side
                other = 11 - index
                start = 0 if step_x < 0 else rows - 2
                land = rows + 2 if step_x < 0 else 0
                src = ypack.at[slot, side, pl.ds(start * DEEP, 2 * DEEP - 1)]
                dst = yslot.at[slot, 1 - side, pl.ds(land * DEEP, 2 * DEEP - 1)]

            @pl.when(there)
            def _():
                pltpu.make_async_remote_copy(
                    src_ref=src, dst_ref=dst, send_sem=send_sem.at[slot, index], recv_sem=recv_sem.at[slot, other],
                    device_id=(my_x + step_x, my_y + step_y), device_id_type=MESH,
                ).start()

    def send_x(source, slot):
        for side in range(2):
            for layer in (1, 2, 3):
                at = layer - 1 if side == 0 else rows - layer
                for c in range(3) if layer < 3 else (0,):
                    e = 3 * (layer - 1) + c
                    xpack[slot, side, pl.ds(e * cols, cols), :] = source[c, pl.ds(at * cols, cols), :]
        for index in (0, 1):
            @pl.when(sides[index][2])
            def _():
                outgoing(index, slot).start()

    near_side = 1 - lax.rem(my_y, 2)

    def pack(source, slot):
        send_y(source, slot, 1 - near_side)
        send_y(source, slot, near_side)
        send_x(source, slot)

    def arrived(index, slot):
        outgoing(index, slot).wait_send()
        outgoing(opposite(index), slot).wait_recv()

    pad[...] = jnp.zeros_like(pad)
    mask_pad[...] = jnp.full_like(mask_pad, -1)
    diagonal[...] = jnp.zeros_like(diagonal)
    for state in (xg, xw, yg, yw, xr, ypack, acc):
        state[...] = jnp.zeros_like(state)
    for state in (mxr, myr, mx3, my3, mypack):
        state[...] = jnp.full_like(state, -1)
    ab[...] = jnp.where(lax.broadcasted_iota(i32, ab.shape, 0) == 0, 1.0, 0.0).astype(f32)
    place = lax.broadcasted_iota(i32, (1, depth), 1)
    fetches[0].wait()
    for word in range(4):
        for r in range(rows):
            mask_pad[word, 3 + r, pl.ds(EDGE, cols), :] = mask[word, pl.ds(r * cols, cols), :]

    for side in range(2):
        for layer in (1, 2):
            at = layer - 1 if side == 0 else cols - layer
            for word in range(4):
                mypack[side, spread(4 * (layer - 1) + word, 8), :] = mask[word, column(at), :]
            at = layer - 1 if side == 0 else rows - layer
            for kept, word in enumerate(FACE_WORDS[1 - side]):
                e = KEPT * (layer - 1) + kept
                mxpack[side, pl.ds(e * cols, cols), :] = mask[word, pl.ds(at * cols, cols), :]
        sign = 1 if side == 0 else -1
        word = bond((0, 3 * sign, 0))[2]
        my3pack[side] = mask[word, column(2 if side == 0 else cols - 3), :]
        word = bond((3 * sign, 0, 0))[2]
        mxpack[side, pl.ds(2 * KEPT * cols, cols), :] = mask[word, pl.ds((2 if side == 0 else rows - 3) * cols, cols), :]

    def own_weights(along):
        for word in range(4):
            mask_shifted[word] = mask_pad[word, :, pl.ds(EDGE + along, cols), :].reshape(-1, depth)
        for upward in range(-3, 4):
            across_all = reach(along, upward)
            if not across_all:
                continue
            inside = (place + upward >= 0) & (place + upward < depth)
            for low in range(0, rows, 4):
                here = pl.ds(low * cols, 4 * cols)
                moments = [None, None, None]
                for across in across_all:
                    word, bit, mirror_word, mirror_bit, weight = bond((across, along, upward))
                    own = mask[word, here] & bit
                    far = mask_shifted[mirror_word, pl.ds((3 + low + across) * cols, 4 * cols)] & mirror_bit
                    far = rolled(jnp.where(far == 0, f32(weight), f32(0.0)), upward)
                    one = jnp.where((own == 0) & inside, far, f32(0.0))
                    weights[NUMBER[(across, along, upward)], here] = one
                    for power in range(3):
                        scale = across**power
                        if scale:
                            moments[power] = add(moments[power], scaled(scale, one))
                for slot, (power, scale) in enumerate((
                    (2, 1), (1, along), (1, upward), (0, along * along), (0, along * upward), (0, upward * upward),
                )):
                    if scale and moments[power] is not None:
                        diagonal[slot, here] += scaled(scale, moments[power])

    for along in range(-3, -3 + EARLY):
        own_weights(along)
    pl.semaphore_wait(barrier, peers)
    for hop in range(1, ny):
        pl.semaphore_signal(ready, inc=1, device_id=(my_x, lax.rem(my_y + hop, ny)), device_id_type=MESH)
    for index in ORDER:
        @pl.when(sides[index][2])
        def _():
            for copy in outgoing_mask(index):
                copy.start()
    fetches[1].wait()
    pack(field, 0)
    fetches[2].wait()
    pack(speed, 1)
    for along in range(-3 + EARLY, 4):
        own_weights(along)

    middle = (slice(None), pl.ds(3, rows), pl.ds(EDGE, cols), slice(None))

    def set_pad(c, value):
        pad[c, pl.ds(3, rows), pl.ds(EDGE, cols), :] = value.reshape(rows, cols, depth)

    def face_weights(axis, side):
        sign = -1 if side == 0 else 1
        terms, powers = {}, {}
        for layer, r in PLANES + LONG:
            for p, c in crossing(layer, r) if (layer, r) in PLANES else [(0, 0)]:
                out = sign * (layer + r)
                offset = (out, p, c) if axis == 0 else (p, out, c)
                word, bit, mirror_word, mirror_bit, weight = bond(offset)
                if axis == 0:
                    at = r if side == 0 else rows - 1 - r
                    own = mask[word, pl.ds(at * cols, cols), :]
                    if layer == 3:
                        far = mx3[side]
                    else:
                        kept = KEPT * (layer - 1) + FACE_WORDS[side].index(mirror_word)
                        far = mxr[side, c + 2, kept, pl.ds(EDGE + p, cols), :]
                else:
                    at = r if side == 0 else cols - 1 - r
                    own = mask[word, column(at), :]
                    if layer == 3:
                        far = my3[side]
                    else:
                        far = myr[side, c + 2, spread((2 + p) * 8 + 4 * (layer - 1) + mirror_word, 8), :]
                one = jnp.where(((own & bit) | (far & mirror_bit)) == 0, f32(weight), f32(0.0))
                if axis == 0:
                    wx[side, FACE[layer, r, p, c]] = one
                else:
                    wy[side, FACE[layer, r, p, c]] = one
                for power in range(3):
                    if p**power:
                        key = (out, r, c, power)
                        powers[key] = add(powers.get(key), scaled(p**power, one))
        for (out, r, c, power), term in powers.items():
            for parts in ((0, 0), (0, 1), (0, 2), (1, 1), (1, 2), (2, 2)):
                tangent = 1 - axis
                if parts.count(tangent) != power:
                    continue
                scale = out ** parts.count(axis) * c ** parts.count(2)
                if scale:
                    key = (r, SLOT[parts])
                    terms[key] = add(terms.get(key), scaled(scale, term))
        for (r, slot), term in terms.items():
            if axis == 0:
                at = r if side == 0 else rows - 1 - r
                diagonal[slot, pl.ds(at * cols, cols), :] += term
            else:
                at = r if side == 0 else cols - 1 - r
                diagonal[slot, column(at), :] += term

    def take_masks(axis):
        for index in range(2) if axis == 0 else range(2, 8):
            step_x, step_y, there = sides[index]

            @pl.when(there)
            def _():
                for copy in outgoing_mask(index):
                    copy.wait_send()
                for copy in outgoing_mask(opposite(index)):
                    copy.wait_recv()
                for upward in range(-2, 3):
                    inside = (place + upward >= 0) & (place + upward < depth)
                    if index < 2:
                        words = mxslot[index, pl.ds(0, 2 * KEPT * cols), :]
                    elif index < 4:
                        first, size = 2 * 8, rows * 8
                        words = myslot[index - 2, pl.ds(first, size), :]
                    else:
                        first, size = (0 if step_x < 0 else (rows + 2) * 8), 16
                        words = myslot[0 if step_y < 0 else 1, pl.ds(first, size), :]
                    if upward:
                        words = jnp.where(inside, rolled(words, upward), -1)
                    if index < 2:
                        mxr[index, upward + 2, :, pl.ds(EDGE, cols), :] = words.reshape(2 * KEPT, cols, depth)
                    else:
                        myr[0 if step_y < 0 else 1, upward + 2, pl.ds(first, size), :] = words
                if index < 2:
                    mx3[index] = mxslot[index, pl.ds(2 * KEPT * cols, cols), :]
                elif index < 4:
                    my3[index - 2] = my3slot[index - 2]
        for side in range(2):
            face_weights(axis, side)

    def own_forces():
        turn = 0
        for low in range(0, rows, 4):
            for c in range(3):
                force[c, pl.ds(low * cols, 4 * cols)] = jnp.zeros((4 * cols, depth), f32)
        for along in range(-3, 4):
            for c in range(3):
                shifted[c] = pad[c, :, pl.ds(EDGE + along, cols), :].reshape(-1, depth)
            for upward in range(-3, 4):
                across_all = reach(along, upward)
                if not across_all:
                    continue
                turn = 1 - turn
                most = max(across_all)
                span = pl.ds(3 * cols, rows * cols)
                if along or upward:
                    mix = None
                    for scale, c in ((along, 1), (upward, 2)):
                        if scale:
                            mix = add(mix, scaled(scale, shifted[c, span]))
                    mixed[turn, span] = rolled(mix, upward)
                if most:
                    plain[turn, span] = rolled(shifted[0, span], upward)
                for low in range(0, rows, 4):
                    here = pl.ds(low * cols, 4 * cols)
                    whole = None
                    lean = None

                    def stretch(across):
                        at = pl.ds((3 + low + across) * cols, 4 * cols)
                        value = mixed[turn, at] if along or upward else None
                        if across:
                            term = float(across) * plain[turn, at]
                            value = term if value is None else value + term
                        return weights[NUMBER[(across, along, upward)], here] * value

                    for across in [a for a in across_all if a >= 0]:
                        if across == 0:
                            whole = stretch(0)
                            continue
                        up, down = stretch(across), stretch(-across)
                        both = up + down
                        whole = both if whole is None else whole + both
                        lean = add(lean, scaled(across, up - down))
                    if lean is not None:
                        force[0, here] += lean
                    if along:
                        force[1, here] += float(along) * whole
                    if upward:
                        force[2, here] += float(upward) * whole

    def diagonal_forces():
        for low in range(0, rows, 4):
            here = pl.ds(low * cols, 4 * cols)
            u = [pad[c, pl.ds(3 + low, 4), pl.ds(EDGE, cols), :].reshape(4 * cols, depth) for c in range(3)]
            d = [diagonal[slot, here] for slot in range(6)]
            force[0, here] -= d[0] * u[0] + d[1] * u[1] + d[2] * u[2]
            force[1, here] -= d[1] * u[0] + d[3] * u[1] + d[4] * u[2]
            force[2, here] -= d[2] * u[0] + d[4] * u[1] + d[5] * u[2]

    def face_forces(axis, side, sign):
        normal, tangent = (0, 1) if axis == 0 else (1, 0)
        result = {}
        for layer in (1, 2):
            inner = [r for one, r in PLANES if one == layer]
            wide = {}
            for c in range(-2, 3):
                sums = {}
                for p in range(-2, 3):
                    targets = [r for r in inner if (layer, r, p, c) in FACE]
                    if not targets:
                        continue

                    def near(component):
                        e = 3 * (layer - 1) + component
                        if axis == 0:
                            return xr[side, c + 2, e, pl.ds(EDGE + p, cols), :]
                        return yr[side, c + 2, spread((2 + p) * DEEP + e), :]

                    out = sign * near(normal)
                    base = None
                    if p:
                        base = scaled(p, near(tangent))
                    if c:
                        base = add(base, scaled(c, near(2)))
                    for r in targets:
                        value = scaled(layer + r, out)
                        if base is not None:
                            value = value + base
                        one = (wx if axis == 0 else wy)[side, FACE[layer, r, p, c]] * value
                        sums[r, 0] = add(sums.get((r, 0)), one)
                        if p:
                            sums[r, 1] = add(sums.get((r, 1)), scaled(p, one))
                for r in inner:
                    if (r, 0) not in sums:
                        continue
                    wide[r, normal] = add(wide.get((r, normal)), sums[r, 0])
                    if (r, 1) in sums:
                        wide[r, tangent] = add(wide.get((r, tangent)), sums[r, 1])
                    if c:
                        wide[r, 2] = add(wide.get((r, 2)), scaled(c, sums[r, 0]))
            for r in inner:
                wide[r, normal] = sign * scaled(layer + r, wide[r, normal])
                for component in range(3):
                    result[r, component] = add(result.get((r, component)), wide[r, component])
        for layer, r in LONG:
            e = 6 if layer == 3 else 3 * (layer - 1) + normal
            if axis == 0:
                out = xg[side, pl.ds(e * cols, cols), :]
            else:
                out = yg[side, spread(2 * DEEP + e), :]
            one = 9.0 * ((wx if axis == 0 else wy)[side, FACE[layer, r, 0, 0]] * out)
            result[r, normal] = add(result.get((r, normal)), one)
        for (r, component), term in result.items():
            if axis == 0:
                at = r if side == 0 else rows - 1 - r
                force[component, pl.ds(at * cols, cols), :] += term
            else:
                at = jnp.where(side == 0, r, cols - 1 - r)
                force[component, column(at), :] += term

    hops = [(hop_x, hop_y) for hop_y in range(ny) for hop_x in range(nx) if hop_x or hop_y]
    hops.sort(key=lambda hop: (abs(2 * hop[1] - ny), abs(2 * hop[0] - nx)))

    def dot(first, second):
        whole = None
        for c in range(3):
            whole = add(whole, jnp.sum((first[c] * second[c]).reshape(-1, 8, depth), axis=0))
        return whole

    def send_sums(slot):
        line = jnp.zeros((1, depth), f32)
        for which in range(6):
            one = jnp.sum(jnp.sum(acc[which], axis=0, keepdims=True), axis=1, keepdims=True)
            line = jnp.where(place == which, one, line)
        sums_out[slot] = line

        for which, (hop_x, hop_y) in enumerate(hops):
            pltpu.make_async_remote_copy(
                src_ref=sums_out.at[slot], dst_ref=sums_in.at[slot, which],
                send_sem=sum_send_sem.at[slot], recv_sem=sum_recv_sem.at[slot],
                device_id=(lax.rem(my_x + hop_x, nx), lax.rem(my_y + hop_y, ny)), device_id_type=MESH,
            ).start()

    def take_sums(slot):
        whole = sums_in.at[slot]
        pltpu.make_async_copy(whole, whole, sum_send_sem.at[slot]).wait()
        pltpu.make_async_copy(whole, whole, sum_recv_sem.at[slot]).wait()
        line = jnp.sum(sums_in[slot], axis=0) + sums_out[slot]
        vv, vg, gg, vw, wg, gh = [
            jnp.sum(jnp.where(place == which, line, 0.0), axis=1, keepdims=True) for which in range(6)
        ]
        alpha, beta = ab[0:1, 0:1], ab[1:2, 0:1]
        kinetic = alpha * alpha * vv + 2.0 * alpha * beta * vg + beta * beta * gg
        rayleigh = -(alpha * alpha * vw + 2.0 * alpha * beta * wg + beta * beta * gh)
        damping = 2.0 * jnp.sqrt(rayleigh / count / (fictive_mass * (kinetic / count + epsilon)))
        alpha = (2.0 - damping) / (2.0 + damping)
        beta = 2.0 / (fictive_mass * (2.0 + damping))
        ab[0:1, :] = jnp.broadcast_to(alpha, (1, depth))
        ab[1:2, :] = jnp.broadcast_to(beta, (1, depth))
        return alpha, beta

    def step(turn, carry):
        @pl.when(turn != 1)
        def _():
            own_forces()

        @pl.when(turn == 0)
        def _():
            take_masks(0)

        @pl.when(turn == 1)
        def _():
            for c in range(3):
                force[c] = change[c]

        sent = lax.rem(turn + 2, SLOTS)
        slot = jnp.where(turn < 3, turn, lax.rem(turn + 1, SLOTS))
        early = turn < 3
        alpha = jnp.where(early, 0.0, ab[0:1, :])
        beta = jnp.where(early, 1.0, ab[1:2, :])
        keep = jnp.where(early, 0.0, jnp.ones((1, depth), f32))

        @pl.when(turn == 3)
        def _():
            for index in range(8):
                step_x, step_y, there = sides[index]

                @pl.when(there)
                def _():
                    arrived(index, 3)
                    if index < 2:
                        xw[index] = xslot[3, index]
                    else:
                        side = 0 if step_y < 0 else 1
                        here = pl.ds(2 * DEEP, rows * DEEP) if index < 4 else pl.ds(0 if step_x < 0 else (rows + 2) * DEEP, 2 * DEEP - 1)
                        yw[side, here] = yslot[3, side, here]

        for index in (0, 1):
            @pl.when(sides[index][2])
            def _():
                arrived(index, slot)
                fresh = alpha * xw[index] + beta * xslot[slot, index]
                xw[index] = fresh
                fresh = keep * xg[index] + fresh
                xg[index] = fresh
                for upward in range(-2, 3):
                    xr[index, upward + 2, :, pl.ds(EDGE, cols), :] = rolled(
                        fresh[: 6 * cols], upward).reshape(6, cols, depth)
        for side in range(2):
            face_forces(0, side, -1.0 if side == 0 else 1.0)

        @pl.when(turn == 0)
        def _():
            take_masks(1)

        diagonal_forces()

        @pl.when(turn == 0)
        def _():
            fetches[3].wait()
            fetches[4].wait()
            for c in range(3):
                force[c] += flags[...].astype(f32) * load[c]

        for side in (near_side, 1 - near_side):
            step_y = 2 * side - 1
            there_y = (my_y + step_y >= 0) & (my_y + step_y < ny)
            for step_x in (0, -1, 1):
                if step_x == 0:
                    there, index, here = there_y, 2 + side, pl.ds(2 * DEEP, rows * DEEP)
                    src = ypack.at[slot, side]
                else:
                    there = there_y & sides[0 if step_x < 0 else 1][2]
                    index = (4 if step_x < 0 else 6) + side
                    here = pl.ds(0 if step_x < 0 else (rows + 2) * DEEP, 2 * DEEP - 1)
                    src = ypack.at[slot, side, pl.ds(0, 2 * DEEP - 1)]

                @pl.when(there)
                def _():
                    copy = pltpu.make_async_remote_copy(
                        src_ref=src, dst_ref=yslot.at[slot, side, here],
                        send_sem=send_sem.at[slot, index], recv_sem=recv_sem.at[slot, index],
                        device_id=(my_x + step_x, my_y + step_y), device_id_type=MESH,
                    )
                    copy.wait_send()
                    copy.wait_recv()
                    fresh = alpha * yw[side, here] + beta * yslot[slot, side, here]
                    yw[side, here] = fresh
                    yg[side, here] = keep * yg[side, here] + fresh
            for upward in range(-2, 3):
                yr[side, upward + 2] = rolled(yg[side], upward)
            face_forces(1, side, jnp.where(side == 0, -1.0, 1.0))

            @pl.when(turn < ITERS)
            def _():
                send_y(force, sent, side)

        @pl.when(turn < ITERS)
        def _():
            send_x(force, sent)

        @pl.when(turn == 0)
        def _():
            for c in range(3):
                total[c] = force[c]
                set_pad(c, speed[c])

        @pl.when(turn == 1)
        def _():
            for c in range(3):
                change[c] = force[c]
                set_pad(c, total[c])
            acc[0] = dot(speed, speed)
            acc[1] = dot(speed, total)
            acc[2] = dot(total, total)
            acc[3] = dot(speed, force)
            acc[4] = dot(force, total)
            pl.semaphore_wait(ready, ny - 1)
            send_sums(0)

        @pl.when(turn >= 2)
        def _():
            acc[5] = dot(total, force)
            send_sums(lax.rem(turn - 1, SLOTS))
            alpha, beta = take_sums(lax.rem(turn - 2, SLOTS))
            sums = [None] * 5
            for c in range(3):
                w = alpha * change[c] + beta * force[c]
                v = alpha * speed[c] + beta * total[c]
                g = total[c] + w
                change[c] = w
                speed[c] = v
                total[c] = g
                field[c] = field[c] + v
                set_pad(c, g)
                for which, (a, b) in enumerate(((v, v), (v, g), (g, g), (v, w), (w, g))):
                    sums[which] = add(sums[which], jnp.sum((a * b).reshape(-1, 8, depth), axis=0))
            for which in range(5):
                acc[which] = sums[which]

        return carry

    for c in range(3):
        set_pad(c, speed[c])
    own_forces()
    for c in range(3):
        change[c] = force[c]
        set_pad(c, field[c])
    lax.fori_loop(0, ITERS + 1, step, 0)
    alpha, beta = take_sums((ITERS - 1) % SLOTS)
    for c in range(3):
        v = alpha * speed[c] + beta * total[c]
        speed[c] = v
        field[c] = field[c] + v


def on_device(nx, ny, disp, vel, load, flags, mask_bits):
    parts, rows, cols, depth = disp.shape
    words = mask_bits.shape[0]
    cells = rows * cols
    f32, i32 = jnp.float32, jnp.int32
    vmem, dma = pltpu.VMEM, pltpu.SemaphoreType.DMA
    wide = cols + 2 * EDGE
    flat = (parts, cells, depth)
    tall = (rows + 6) * cols
    ring = (rows + 4) * 8
    deep = (rows + 4) * DEEP
    scratch = [
        vmem(flat, f32),
        vmem((cells, depth), i32),
        vmem((words, cells, depth), i32),
        vmem((len(TABLE), cells, depth), f32),
        vmem((6, cells, depth), f32),
        vmem((parts, rows + 6, wide, depth), f32),
        vmem((words, rows + 6, wide, depth), i32),
        vmem((parts, tall, depth), f32),
        vmem((words, tall, depth), i32),
        vmem((2, tall, depth), f32),
        vmem((2, tall, depth), f32),
        vmem(flat, f32),
        vmem(flat, f32),
        vmem(flat, f32),
        vmem((2, len(FACE), cols, depth), f32),
        vmem((2, len(FACE), rows, depth), f32),
        vmem((2, 7 * cols, depth), f32),
        vmem((2, 7 * cols, depth), f32),
        vmem((2, deep, depth), f32),
        vmem((2, deep, depth), f32),
        vmem((2, 5, 6, wide, depth), f32),
        vmem((2, 5, deep, depth), f32),
        vmem((2, 5, 2 * KEPT, wide, depth), i32),
        vmem((2, 5, ring, depth), i32),
        vmem((2, cols, depth), i32),
        vmem((2, rows, depth), i32),
        vmem((SLOTS, 2, 7 * cols, depth), f32),
        vmem((SLOTS, 2, rows * DEEP, depth), f32),
        vmem((SLOTS, 2, 7 * cols, depth), f32),
        vmem((SLOTS, 2, deep, depth), f32),
        vmem((2, (2 * KEPT + 1) * cols, depth), i32),
        vmem((2, rows * 8, depth), i32),
        vmem((2, rows, depth), i32),
        vmem((2, (2 * KEPT + 1) * cols, depth), i32),
        vmem((2, ring, depth), i32),
        vmem((2, rows, depth), i32),
        vmem((6, 8, depth), f32),
        vmem((8, depth), f32),
        vmem((SLOTS, 1, depth), f32),
        vmem((SLOTS, nx * ny - 1, 1, depth), f32),
        dma((5,)),
        dma((SLOTS, 8)),
        dma((SLOTS, 8)),
        dma((2, 8)),
        dma((2, 8)),
        dma((SLOTS,)),
        dma((SLOTS,)),
        pltpu.SemaphoreType.REGULAR,
    ]
    outs = pl.pallas_call(
        functools.partial(kernel, nx, ny),
        out_shape=[jax.ShapeDtypeStruct(flat, f32)] * 2,
        in_specs=[pl.BlockSpec(memory_space=pltpu.HBM)] * 5,
        out_specs=[pl.BlockSpec(memory_space=pltpu.VMEM)] * 2,
        scratch_shapes=scratch,
        compiler_params=pltpu.CompilerParams(
            has_side_effects=True, collective_id=0, vmem_limit_bytes=67043328),
    )(disp.reshape(flat), vel.reshape(flat), load.reshape(flat), flags.reshape(cells, depth),
      mask_bits.reshape(words, cells, depth))
    return tuple(out.reshape(disp.shape) for out in outs)


def solution(mesh):
    cells = P(None, "gx", "gy", None)
    return jax.shard_map(
        functools.partial(on_device, mesh.shape["gx"], mesh.shape["gy"]),
        mesh=mesh,
        in_specs=(cells, cells, cells, P("gx", "gy", None), cells),
        out_specs=(cells, cells),
        check_vma=False,
    )
```
